32 devices in a mesh: dp: 1 (over z), pz: 4 (over y), py: 8 (over x, core).
Axes of the slice: x: 4, y: 4, z: 1, core: 2. Of those that a mesh axis runs over, the one named last changes fastest.
The devices are a block of a 4x4x8 slice.
Arguments:
- rho_re: float32 [2, 256, 256, 256], P('dp', None, 'py', 'pz')
- rho_im: float32 [2, 256, 256, 256], P('dp', None, 'py', 'pz')
- g_re: float32 [256, 256, 256], P('py', 'pz')
- g_im: float32 [256, 256, 256], P('py', 'pz')
Outputs:
- output 1: float32 [2, 256, 256, 256], P('dp', None, 'py', 'pz')
- output 2: float32 [2, 256, 256, 256], P('dp', None, 'py', 'pz')
- output 3: float32 [2, 256, 256, 256], P('dp', 'py', 'pz')
- output 4: float32 [2, 256, 256, 256], P('dp', 'py', 'pz')
All inputs are finite; a program needn't handle non-finite values.
Results may differ from the reference program's by a relative error of at most 0.001.
Values sent between devices are 32-bit elements.
A program may use at most 768 MiB of HBM per device.

```python
import jax
import jax.numpy as jnp
from jax import lax

GRID = 256
FIELDS = 2


def green_kernel():
    positions = jnp.arange(GRID)
    wavenum = jnp.where(positions < (GRID + 1) // 2, positions, positions - GRID).astype(jnp.float32)
    wave_sq = wavenum * wavenum * (16.0 / (GRID * GRID))
    return 1.0 / (1.0 + wave_sq[:, None, None] + 2.0 * wave_sq[None, :, None] + 3.0 * wave_sq[None, None, :])


def setup_inputs(seed: int = 0, part: int = 0) -> dict:
    part_key = jax.random.fold_in(jax.random.key(seed), part)
    key_re, key_im = jax.random.split(part_key)
    field_shape = (FIELDS, GRID, GRID, GRID)
    rho_re = jax.random.normal(key_re, field_shape, jnp.float32)
    rho_im = jax.random.normal(key_im, field_shape, jnp.float32)
    green_re_key, green_im_key = jax.random.split(jax.random.key(seed + 1))
    kernel = green_kernel()
    g_re = kernel * (1.0 + 0.5 * jax.random.normal(green_re_key, kernel.shape, jnp.float32))
    g_im = kernel * (0.5 * jax.random.normal(green_im_key, kernel.shape, jnp.float32))
    return {"rho_re": rho_re, "rho_im": rho_im, "g_re": g_re, "g_im": g_im}


def reference(rho_re, rho_im, g_re, g_im):
    green_fn = lax.complex(g_re, g_im)

    def one_field(field_pair):
        volume = lax.complex(field_pair[0], field_pair[1])
        spectrum = jnp.fft.fftn(volume, axes=(0, 1, 2), norm="ortho") * green_fn
        restored = jnp.fft.ifftn(spectrum, axes=(0, 1, 2), norm="ortho")
        return jnp.real(restored), jnp.imag(restored), jnp.real(spectrum), jnp.imag(spectrum)

    phi_re, phi_im, hat_re, hat_im = lax.map(one_field, (rho_re, rho_im))
    return (phi_re, phi_im, hat_re, hat_im)
```

```python
import functools

import jax
import jax.numpy as jnp
import numpy as np
from jax import lax
from jax.experimental import pallas as pl
from jax.experimental.pallas import tpu as pltpu
from jax.sharding import PartitionSpec as P

MESH = pl.DeviceIdType.MESH
HALF_X_CHUNKS = 4
LANES = 128


def real_form(matrix):
    return np.block([[matrix.real, -matrix.imag], [matrix.imag, matrix.real]])


def dft_tables(n, ny, nz):
    half = n // 2
    scale = 1.0 / np.sqrt(n)
    low, full = np.arange(half), np.arange(n)
    dft = lambda k, j, sign: scale * np.exp(sign * 2j * np.pi * ((k[:, None] * j[None, :]) % n) / n)
    per = n // ny // HALF_X_CHUNKS // 2
    order = np.arange(half).reshape(ny, HALF_X_CHUNKS, per).transpose(1, 0, 2)
    rows = np.stack([order, order + half], axis=2).reshape(-1)
    wx = np.stack([real_form(dft(2 * low + p, low, -1))[rows] for p in range(2)])
    wxi = np.stack([real_form(dft(low, 2 * low + p, 1))[:, rows].T for p in range(2)])
    wy = np.stack([real_form(dft(2 * low + p, low, -1)) for p in range(2)])
    wyi = np.stack([real_form(dft(low, 2 * low + p, 1)) for p in range(2)])
    lz = n // nz
    zrows = np.arange(n).reshape(nz, lz)
    zrows = np.stack([zrows, zrows + n], axis=1).reshape(-1)
    wz = real_form(dft(full, full, -1)).T[zrows]
    wzi = real_form(dft(full, full, 1)).T[:, zrows]
    return [np.asarray(w, np.float32) for w in (wx, wy, wz, wzi, wyi, wxi)]


def dot(a, b, dims=((1,), (0,))):
    return lax.dot_general(a, b, (dims, ((), ())), precision=lax.Precision.HIGHEST,
                           preferred_element_type=jnp.float32)


def kernel(ny, nz, n, nf,
           rho_re, rho_im, g_re, g_im, wx_h, wy_h, wz_h, wzi_h, wyi_h, wxi_h,
           phi_re, phi_im, hat_re, hat_im,
           abuf, bbuf, cbuf, dbuf, ebuf, even, stage, gbuf, hbuf, wx, wy, wz, wzi, wyi, wxi,
           xs, xr, ys, yr, yis, yir, xis, xir, w_sem, in_sem, g_sem, h_sem):
    py, pz = lax.axis_index("py"), lax.axis_index("pz")
    half = n // 2
    yl, zl = n // ny, n // nz
    kc = n // ny // HALF_X_CHUNKS // 2
    nj = 2 * HALF_X_CHUNKS
    xrow, yrow = yl * 2 * kc, 2 * kc * zl
    crow = ny * xrow
    rho, phi, gg, hat = (rho_re, rho_im), (phi_re, phi_im), (g_re, g_im), (hat_re, hat_im)
    x_offsets = (4, 3, 5, 2, 6, 1, 7) if ny == 8 else tuple(range(1, ny))
    y_offsets = (2, 1, 3) if nz == 4 else tuple(range(1, nz))

    barrier = pltpu.get_barrier_semaphore()
    for o in range(1, ny):
        pl.semaphore_signal(barrier, inc=1, device_id={"py": lax.rem(py + o, ny)}, device_id_type=MESH)
    for o in range(1, nz):
        pl.semaphore_signal(barrier, inc=1, device_id={"pz": lax.rem(pz + o, nz)}, device_id_type=MESH)

    tables = [pltpu.make_async_copy(h, v, w_sem.at[i]) for i, (h, v) in enumerate(
        ((wx_h, wx), (wy_h, wy), (wz_h, wz), (wzi_h, wzi), (wyi_h, wyi), (wxi_h, wxi)))]

    def rho_copy(c, pair, slot):
        return pltpu.make_async_copy(rho[c].at[:, pl.ds(2 * pair, 2)], stage.at[slot, c], in_sem.at[slot, c])

    def phi_copy(c, pair, slot):
        return pltpu.make_async_copy(stage.at[slot, c], phi[c].at[:, pl.ds(2 * pair, 2)], in_sem.at[slot, c])

    def g_copy(c, j):
        p, jj, slot = j // HALF_X_CHUNKS, lax.rem(j, HALF_X_CHUNKS), lax.rem(j, 2)
        return pltpu.make_async_copy(gg[c].at[pl.ds(kc * jj, kc), p], gbuf.at[slot, c], g_sem.at[slot, c])

    def hat_copy(c, f, j):
        p, jj, slot = j // HALF_X_CHUNKS, lax.rem(j, HALF_X_CHUNKS), lax.rem(j, 2)
        return pltpu.make_async_copy(hbuf.at[slot, c, f], hat[c].at[f, pl.ds(kc * jj, kc), p], h_sem.at[slot, c, f])

    def x_copy(src, dst, ss, rs, j, o):
        to = lax.rem(py + o, ny)
        return pltpu.make_async_remote_copy(
            src.at[pl.ds(pl.multiple_of(j * crow + to * xrow, 8), xrow)],
            dst.at[pl.ds(pl.multiple_of(j * crow + py * xrow, 8), xrow)],
            ss.at[j, o - 1], rs.at[j, o - 1], device_id={"py": to}, device_id_type=MESH)

    def y_copy(src, dst, ss, rs, j, o):
        to = lax.rem(pz + o, nz)
        return pltpu.make_async_remote_copy(
            src.at[pl.ds(pl.multiple_of(j * crow + to * yrow, 8), yrow)],
            dst.at[pl.ds(pl.multiple_of(j * crow + pz * yrow, 8), yrow)],
            ss.at[j, o - 1], rs.at[j, o - 1], device_id={"pz": to}, device_id_type=MESH)

    def own(src, dst, j, mine, rows):
        at = pl.ds(pl.multiple_of(j * crow + mine * rows, 8), rows)
        dst[at, :] = src[at, :]

    xf = functools.partial(x_copy, abuf, bbuf, xs, xr)
    yf = functools.partial(y_copy, abuf, cbuf, ys, yr)
    yi = functools.partial(y_copy, cbuf, dbuf, yis, yir)
    xi = functools.partial(x_copy, bbuf, ebuf, xis, xir)

    def x_forward(p):
        for c in range(2):
            rho_copy(c, 0, 0).start()

        def body(pair, carry):
            slot = lax.rem(pair, 2)
            for c in range(2):
                rho_copy(c, pair, slot).wait()

            @pl.when(pair + 1 < yl // 2)
            def _():
                for c in range(2):
                    rho_copy(c, pair + 1, 1 - slot).start()

            folded = []
            for c in range(2):
                lines = stage[slot, c]
                first, second = lines[..., :half], lines[..., half:]
                both = first - second if p else first + second
                folded.append(jnp.swapaxes(both, 0, 1).reshape(2 * nf * zl, half))
            out = dot(wx[p], jnp.concatenate(folded, axis=1), ((1,), (1,)))
            for jj in range(HALF_X_CHUNKS):
                for to in range(ny):
                    r = (jj * ny + to) * 2 * kc
                    for y in range(2):
                        at = (p * HALF_X_CHUNKS + jj) * crow + to * xrow + (2 * pair + y) * 2 * kc
                        abuf[pl.ds(pl.multiple_of(at, 8), 2 * kc), :] = out[r:r + 2 * kc, y * LANES:(y + 1) * LANES]
            return carry

        lax.fori_loop(0, yl // 2, body, 0)

    def x_send(p):
        for jj in range(HALF_X_CHUNKS):
            j = p * HALF_X_CHUNKS + jj
            for o in x_offsets:
                xf(j, o).start()

    def y_forward(j):
        own(abuf, bbuf, j, py, xrow)
        base = j * crow
        for i0 in range(0, kc, 2):
            parts = []
            for c in range(2):
                parts.append(jnp.concatenate(
                    [bbuf[pl.ds(base + c * kc + i, n, stride=2 * kc), :] for i in (i0, i0 + 1)], axis=1))
            for p in range(2):
                folded = jnp.concatenate([v[:half] - v[half:] if p else v[:half] + v[half:] for v in parts], axis=0)
                out = dot(wy[p], folded)
                for c in range(2):
                    for to in range(nz):
                        for k in range(2):
                            at = base + to * yrow + (c * kc + i0 + k) * zl + p
                            abuf[pl.ds(at, zl // 2, stride=2), :] = out[
                                c * half + to * zl // 2:c * half + (to + 1) * zl // 2, k * LANES:(k + 1) * LANES]

    def z_solve(j):
        own(abuf, cbuf, j, pz, yrow)
        base, slot = j * crow, lax.rem(j, 2)
        rows = kc * zl
        left = lax.broadcasted_iota(jnp.int32, (rows, LANES), 1) < zl
        swap = lambda v: pltpu.roll(v, zl, 1)
        lines = ([], [])
        for b in range(nz):
            at = base + b * yrow
            re = cbuf[pl.ds(pl.multiple_of(at, 8), rows), :]
            im = cbuf[pl.ds(pl.multiple_of(at + rows, 8), rows), :]
            lines[0].append(jnp.where(left, re, swap(im)))
            lines[1].append(jnp.where(left, swap(re), im))
        gr = gbuf[slot, 0].reshape(rows, n)
        gi = gbuf[slot, 1].reshape(rows, n)
        back = []
        for f in range(nf):
            spec = dot(jnp.concatenate(lines[f], axis=1), wz[...])
            sr, si = spec[:, :n], spec[:, n:]
            hr, hi = sr * gr - si * gi, sr * gi + si * gr
            hbuf[slot, 0, f] = hr.reshape(kc, zl, n)
            hbuf[slot, 1, f] = hi.reshape(kc, zl, n)
            back.append(dot(jnp.concatenate([hr, hi], axis=1), wzi[...]))
        for b in range(nz):
            first, second = (v[:, b * LANES:(b + 1) * LANES] for v in back)
            at = base + b * yrow
            cbuf[pl.ds(pl.multiple_of(at, 8), rows), :] = jnp.where(left, first, swap(second))
            cbuf[pl.ds(pl.multiple_of(at + rows, 8), rows), :] = jnp.where(left, swap(first), second)

    def y_inverse(j):
        own(cbuf, dbuf, j, pz, yrow)
        base = j * crow
        for i0 in range(0, kc, 2):
            halves = []
            for p in range(2):
                lines = []
                for k in range(2):
                    lines.append(jnp.concatenate(
                        [dbuf[pl.ds(base + src * yrow + (c * kc + i0 + k) * zl + p, zl // 2, stride=2), :]
                         for c in range(2) for src in range(nz)], axis=0))
                halves.append(dot(wyi[p], jnp.concatenate(lines, axis=1)))
            for s, out in enumerate((halves[0] + halves[1], halves[0] - halves[1])):
                for c in range(2):
                    for k in range(2):
                        at = base + s * (ny // 2) * xrow + c * kc + i0 + k
                        bbuf[pl.ds(at, half, stride=2 * kc), :] = out[
                            c * half:(c + 1) * half, k * LANES:(k + 1) * LANES]

    def x_gather(p, pair):
        lines = []
        for y in range(2):
            lines.append(jnp.concatenate(
                [ebuf[pl.ds(pl.multiple_of((p * HALF_X_CHUNKS + jj) * crow + src * xrow + (2 * pair + y) * 2 * kc, 8),
                            2 * kc), :]
                 for jj in range(HALF_X_CHUNKS) for src in range(ny)], axis=0))
        return dot(jnp.concatenate(lines, axis=1), wxi[p], ((0,), (0,)))

    for table in tables:
        table.start()
    for c in range(2):
        g_copy(c, 0).start()
        g_copy(c, 1).start()
    tables[0].wait()
    x_forward(0)
    pl.semaphore_wait(barrier, ny + nz - 2)
    x_send(0)
    x_forward(1)
    x_send(1)
    for table in tables[1:]:
        table.wait()

    def step(t, carry):
        @pl.when(t < nj)
        def _():
            for o in x_offsets:
                xf(t, o).wait()
            y_forward(t)
            for o in y_offsets:
                yf(t, o).start()

        @pl.when((t >= 1) & (t < nj + 1))
        def _():
            j = t - 1
            for o in y_offsets:
                yf(j, o).wait()
            for c in range(2):
                g_copy(c, j).wait()

            @pl.when(j >= 2)
            def _():
                for c in range(2):
                    for f in range(nf):
                        hat_copy(c, f, j - 2).wait()

            z_solve(j)
            for o in y_offsets:
                yi(j, o).start()
            for c in range(2):
                for f in range(nf):
                    hat_copy(c, f, j).start()

            @pl.when(j + 2 < nj)
            def _():
                for c in range(2):
                    g_copy(c, j + 2).start()

        @pl.when(t >= 2)
        def _():
            j = t - 2
            for o in y_offsets:
                yi(j, o).wait()
            y_inverse(j)
            for o in x_offsets:
                xi(j, o).start()
            own(bbuf, ebuf, j, py, xrow)

        @pl.when(t == nj)
        def _():
            for jj in range(HALF_X_CHUNKS):
                for o in x_offsets:
                    xi(jj, o).wait()

            def body(pair, c):
                even[pair] = x_gather(0, pair)
                return c

            lax.fori_loop(0, yl // 2, body, 0)

        return carry

    lax.fori_loop(0, nj + 2, step, 0)
    for jj in range(HALF_X_CHUNKS, nj):
        for o in x_offsets:
            xi(jj, o).wait()

    def finish(pair, carry):
        slot = lax.rem(pair, 2)

        @pl.when(pair >= 2)
        def _():
            for c in range(2):
                phi_copy(c, pair - 2, slot).wait()

        e, o = even[pair], x_gather(1, pair)
        for c in range(2):
            er, orr = e[:, c * half:(c + 1) * half], o[:, c * half:(c + 1) * half]
            out = jnp.concatenate([er + orr, er - orr], axis=1).reshape(2, nf, zl, n)
            stage[slot, c] = jnp.swapaxes(out, 0, 1)
            phi_copy(c, pair, slot).start()
        return carry

    lax.fori_loop(0, yl // 2, finish, 0)
    for pair in (yl // 2 - 2, yl // 2 - 1):
        for c in range(2):
            phi_copy(c, pair, pair % 2).wait()
    for j in (nj - 2, nj - 1):
        for c in range(2):
            for f in range(nf):
                hat_copy(c, f, j).wait()


def solution(mesh):
    ny, nz = mesh.shape["py"], mesh.shape["pz"]

    def local_solve(rho_re, rho_im, g_re, g_im):
        nf, n, yl, zl = rho_re.shape
        kl, ml = g_re.shape[:2]
        kc = kl // HALF_X_CHUNKS // 2
        nj = 2 * HALF_X_CHUNKS
        rows = nj * ny * yl * 2 * kc
        tables = [jnp.asarray(w) for w in dft_tables(n, ny, nz)]
        space = jax.ShapeDtypeStruct((nf, yl, zl, n), jnp.float32)
        wave = jax.ShapeDtypeStruct((nf, kl // 2, 2, ml, n), jnp.float32)
        dma = pltpu.SemaphoreType.DMA
        buf = pltpu.VMEM((rows, LANES), jnp.float32)
        outs = pl.pallas_call(
            functools.partial(kernel, ny, nz, n, nf),
            out_shape=(space, space, wave, wave),
            in_specs=[pl.BlockSpec(memory_space=pl.ANY)] * 10,
            out_specs=[pl.BlockSpec(memory_space=pl.ANY)] * 4,
            scratch_shapes=[
                buf, buf, buf, buf, buf,
                pltpu.VMEM((yl // 2, 2 * nf * zl, n), jnp.float32),
                pltpu.VMEM((2, 2, nf, 2, zl, n), jnp.float32),
                pltpu.VMEM((2, 2, kc, ml, n), jnp.float32),
                pltpu.VMEM((2, 2, nf, kc, ml, n), jnp.float32),
                *[pltpu.VMEM(t.shape, jnp.float32) for t in tables],
                dma((nj, ny - 1)), dma((nj, ny - 1)), dma((nj, nz - 1)), dma((nj, nz - 1)),
                dma((nj, nz - 1)), dma((nj, nz - 1)), dma((nj, ny - 1)), dma((nj, ny - 1)),
                dma((len(tables),)), dma((2, 2)), dma((2, 2)), dma((2, 2, nf)),
            ],
            compiler_params=pltpu.CompilerParams(
                collective_id=0, has_side_effects=True, vmem_limit_bytes=67043328),
            name="spectral",
        )(jnp.transpose(rho_re, (0, 2, 3, 1)), jnp.transpose(rho_im, (0, 2, 3, 1)),
          g_re.reshape(kl // 2, 2, ml, n), g_im.reshape(kl // 2, 2, ml, n), *tables)
        phi = [jnp.transpose(v, (0, 3, 1, 2)) for v in outs[:2]]
        return (*phi, *(v.reshape(nf, kl, ml, n) for v in outs[2:]))

    space_layout = P("dp", None, "py", "pz")
    wave_layout = P("dp", "py", "pz", None)
    green_layout = P("py", "pz", None)
    return jax.shard_map(local_solve, mesh=mesh,
                         in_specs=(space_layout, space_layout, green_layout, green_layout),
                         out_specs=(space_layout, space_layout, wave_layout, wave_layout),
                         check_vma=False)
```

```python
import functools

import jax
import jax.numpy as jnp
import numpy as np
from jax import lax
from jax.experimental import pallas as pl
from jax.experimental.pallas import tpu as pltpu
from jax.sharding import PartitionSpec as P

MESH = pl.DeviceIdType.MESH
HALF_X_CHUNKS = 8
SLOTS = 4
LANES = 128
INNER_VMEM = 42 << 20


def real_form(matrix):
    return np.block([[matrix.real, -matrix.imag], [matrix.imag, matrix.real]])


def dft_tables(n, ny, nz):
    half = n // 2
    scale = 1.0 / np.sqrt(n)
    low, full = np.arange(half), np.arange(n)
    dft = lambda k, j, sign: scale * np.exp(sign * 2j * np.pi * ((k[:, None] * j[None, :]) % n) / n)
    per = n // ny // HALF_X_CHUNKS // 2
    order = np.arange(half).reshape(ny, HALF_X_CHUNKS, per).transpose(1, 0, 2)
    rows = np.stack([order, order + half], axis=2).reshape(-1)
    wx = np.stack([real_form(dft(2 * low + p, low, -1))[rows] for p in range(2)])
    wxi = np.stack([real_form(dft(low, 2 * low + p, 1))[:, rows].T for p in range(2)])
    wy = np.stack([real_form(dft(2 * low + p, low, -1)) for p in range(2)])
    wyi = np.stack([real_form(dft(low, 2 * low + p, 1)) for p in range(2)])
    lz = n // nz
    zrows = np.arange(n).reshape(nz, lz)
    zrows = np.stack([zrows, zrows + n], axis=1).reshape(-1)
    wz = real_form(dft(full, full, -1)).T[zrows]
    wzi = real_form(dft(full, full, 1)).T[:, zrows]
    return [np.asarray(w, np.float32) for w in (wx, wy, wz, wzi, wyi, wxi)]


def dot(a, b, dims=((1,), (0,))):
    return lax.dot_general(a, b, (dims, ((), ())), precision=lax.Precision.HIGHEST,
                           preferred_element_type=jnp.float32)


def swap_rows(first, second):
    a, b = first.reshape(-1, 8, LANES), second.reshape(-1, 8, LANES)
    upper = lax.broadcasted_iota(jnp.int32, a.shape, 1) < 4
    return jnp.where(upper, a, pltpu.roll(b, 4, 1)), jnp.where(upper, pltpu.roll(a, 4, 1), b)


def kernel(ny, nz, n, nf,
           rho_re, rho_im, g_re, g_im, wx_h, wy_h, wz_h, wzi_h, wyi_h, wxi_h,
           ebuf, even, hat_re, hat_im,
           abuf, bbuf, cbuf, dbuf, stage, gbuf, wx, wy, wz, wzi, wyi, wxi,
           xs, xr, ys, yr, yis, yir, xis, xir, w_sem, in_sem, g_sem):
    py, pz = lax.axis_index("py"), lax.axis_index("pz")
    half = n // 2
    yl, zl = n // ny, n // nz
    kc = n // ny // HALF_X_CHUNKS // 2
    nj = 2 * HALF_X_CHUNKS
    xrow, yrow = yl * 2 * kc, 2 * kc * zl
    crow = ny * xrow
    pairs = yl // 2
    quarter = pairs // 4
    rho, gg, hat = (rho_re, rho_im), (g_re, g_im), (hat_re, hat_im)
    x_offsets = (4, 3, 5, 2, 6, 1, 7) if ny == 8 else tuple(range(1, ny))
    y_offsets = (2, 1, 3) if nz == 4 else tuple(range(1, nz))

    barrier = pltpu.get_barrier_semaphore()
    for o in range(1, ny):
        pl.semaphore_signal(barrier, inc=1, device_id={"py": lax.rem(py + o, ny)}, device_id_type=MESH)
    for o in range(1, nz):
        pl.semaphore_signal(barrier, inc=1, device_id={"pz": lax.rem(pz + o, nz)}, device_id_type=MESH)

    tables = [pltpu.make_async_copy(h, v, w_sem.at[i]) for i, (h, v) in enumerate(
        ((wx_h, wx), (wy_h, wy), (wz_h, wz), (wzi_h, wzi), (wyi_h, wyi), (wxi_h, wxi)))]

    def rho_copy(c, pair):
        slot = lax.rem(pair, SLOTS)
        return pltpu.make_async_copy(rho[c].at[:, pl.ds(2 * pair, 2)], stage.at[slot, c], in_sem.at[slot, c])

    def g_copy(c, j):
        p, jj, slot = j // HALF_X_CHUNKS, lax.rem(j, HALF_X_CHUNKS), lax.rem(j, 2)
        return pltpu.make_async_copy(gg[c].at[pl.ds(kc * jj, kc), p], gbuf.at[slot, c], g_sem.at[slot, c])

    def x_copy(src, dst, ss, rs, j, o, first=0, count=None):
        to = lax.rem(py + o, ny)
        rows = xrow if count is None else count
        return pltpu.make_async_remote_copy(
            src.at[pl.ds(pl.multiple_of(j * crow + to * xrow + first, 8), rows)],
            dst.at[pl.ds(pl.multiple_of(j * crow + py * xrow + first, 8), rows)],
            ss.at[j], rs.at[j], device_id={"py": to}, device_id_type=MESH)

    def y_copy(src, dst, ss, rs, j, o):
        to = lax.rem(pz + o, nz)
        return pltpu.make_async_remote_copy(
            src.at[pl.ds(pl.multiple_of(j * crow + to * yrow, 8), yrow)],
            dst.at[pl.ds(pl.multiple_of(j * crow + pz * yrow, 8), yrow)],
            ss.at[j], rs.at[j], device_id={"pz": to}, device_id_type=MESH)

    def await_all(src, dst, ss, rs, j, axis, me, size, rows):
        at = pl.ds(pl.multiple_of(j * crow, 8), rows)
        pltpu.make_async_remote_copy(src.at[at], dst.at[at], ss.at[j], rs.at[j],
                                     device_id={axis: lax.rem(me + 1, size)}, device_id_type=MESH).wait()

    def own(src, dst, j, mine, rows):
        at = pl.ds(pl.multiple_of(j * crow + mine * rows, 8), rows)
        dst[at, :] = src[at, :]

    xf = functools.partial(x_copy, abuf, bbuf, xs, xr)
    yf = functools.partial(y_copy, abuf, cbuf, ys, yr)
    yi = functools.partial(y_copy, cbuf, dbuf, yis, yir)
    xi = functools.partial(x_copy, bbuf, ebuf, xis, xir)
    xf_wait = lambda j: await_all(abuf, bbuf, xs, xr, j, "py", py, ny, (ny - 1) * xrow)
    yf_wait = lambda j: await_all(abuf, cbuf, ys, yr, j, "pz", pz, nz, (nz - 1) * yrow)
    yi_wait = lambda j: await_all(cbuf, dbuf, yis, yir, j, "pz", pz, nz, (nz - 1) * yrow)
    xi_wait = lambda j: await_all(bbuf, ebuf, xis, xir, j, "py", py, ny, (ny - 1) * xrow)

    def x_prefetch(first):
        for k in range(SLOTS - 1):
            for c in range(2):
                rho_copy(c, first + k).start()

    def x_forward(p, first, stop):
        def body(pair, carry):
            @pl.when(pair + SLOTS - 1 < stop)
            def _():
                for c in range(2):
                    rho_copy(c, pair + SLOTS - 1).start()

            for c in range(2):
                rho_copy(c, pair).wait()
            slot = lax.rem(pair, SLOTS)
            folded = []
            for c in range(2):
                lines = stage[slot, c]
                low, high = lines[..., :half], lines[..., half:]
                both = low - high if p else low + high
                folded.append(jnp.swapaxes(both, 0, 1).reshape(2 * nf * zl, half))
            out = dot(wx[p], jnp.concatenate(folded, axis=1), ((1,), (1,)))
            blocks = swap_rows(out[:, :LANES], out[:, LANES:])
            for jj in range(HALF_X_CHUNKS):
                for to in range(ny):
                    r = jj * ny + to
                    at = (p * HALF_X_CHUNKS + jj) * crow + to * xrow + pair * 8
                    abuf[pl.ds(pl.multiple_of(at, 8), 8), :] = blocks[r % 2][r // 2]
            if p == 0:
                @pl.when(lax.rem(pair, quarter) == quarter - 1)
                def _():
                    for o in x_offsets:
                        xf(0, o, (pair - (quarter - 1)) * 8, quarter * 8).start()
            return carry

        lax.fori_loop(first, stop, body, 0)

    def y_forward(j):
        own(abuf, bbuf, j, py, xrow)
        base = j * crow
        parts = []
        for c in range(2):
            parts.append(jnp.concatenate(
                [bbuf[pl.ds(base + c * kc + i, n, stride=2 * kc), :] for i in range(2)], axis=1))
        for p in range(2):
            folded = jnp.concatenate([v[:half] - v[half:] if p else v[:half] + v[half:] for v in parts], axis=0)
            out = dot(wy[p], folded)
            for c in range(2):
                for to in range(nz):
                    for k in range(2):
                        at = base + to * yrow + (c * kc + k) * zl + p
                        abuf[pl.ds(at, zl // 2, stride=2), :] = out[
                            c * half + to * zl // 2:c * half + (to + 1) * zl // 2, k * LANES:(k + 1) * LANES]

    def z_solve(j):
        own(abuf, cbuf, j, pz, yrow)
        base, slot = j * crow, lax.rem(j, 2)
        p, jj = j // HALF_X_CHUNKS, lax.rem(j, HALF_X_CHUNKS)
        rows = kc * zl
        left = lax.broadcasted_iota(jnp.int32, (rows, LANES), 1) < zl
        swap = lambda v: pltpu.roll(v, zl, 1)
        lines = ([], [])
        for b in range(nz):
            at = base + b * yrow
            re = cbuf[pl.ds(pl.multiple_of(at, 8), rows), :]
            im = cbuf[pl.ds(pl.multiple_of(at + rows, 8), rows), :]
            lines[0].append(jnp.where(left, re, swap(im)))
            lines[1].append(jnp.where(left, swap(re), im))
        both = jnp.concatenate([jnp.concatenate(v, axis=1) for v in lines], axis=0)
        spec = dot(both, wz[...])
        gr = gbuf[slot, 0].reshape(rows, n)
        gi = gbuf[slot, 1].reshape(rows, n)
        scaled = []
        for f in range(nf):
            sr, si = spec[f * rows:(f + 1) * rows, :n], spec[f * rows:(f + 1) * rows, n:]
            hr, hi = sr * gr - si * gi, sr * gi + si * gr
            hat_re[f, pl.ds(kc * jj, kc), p] = hr.reshape(kc, zl, n)
            hat_im[f, pl.ds(kc * jj, kc), p] = hi.reshape(kc, zl, n)
            scaled.append(jnp.concatenate([hr, hi], axis=1))
        back = dot(jnp.concatenate(scaled, axis=0), wzi[...])
        for b in range(nz):
            first, second = (back[f * rows:(f + 1) * rows, b * LANES:(b + 1) * LANES] for f in range(2))
            at = base + b * yrow
            cbuf[pl.ds(pl.multiple_of(at, 8), rows), :] = jnp.where(left, first, swap(second))
            cbuf[pl.ds(pl.multiple_of(at + rows, 8), rows), :] = jnp.where(left, swap(first), second)

    def y_inverse(j):
        own(cbuf, dbuf, j, pz, yrow)
        base = j * crow
        halves = []
        for p in range(2):
            lines = []
            for k in range(2):
                lines.append(jnp.concatenate(
                    [dbuf[pl.ds(base + src * yrow + (c * kc + k) * zl + p, zl // 2, stride=2), :]
                     for c in range(2) for src in range(nz)], axis=0))
            halves.append(dot(wyi[p], jnp.concatenate(lines, axis=1)))
        for s, out in enumerate((halves[0] + halves[1], halves[0] - halves[1])):
            for c in range(2):
                for k in range(2):
                    at = base + s * (ny // 2) * xrow + c * kc + k
                    bbuf[pl.ds(at, half, stride=2 * kc), :] = out[
                        c * half:(c + 1) * half, k * LANES:(k + 1) * LANES]

    x_prefetch(0)
    tables[0].start()
    for c in range(2):
        g_copy(c, 0).start()
        g_copy(c, 1).start()
    for table in tables[1:]:
        table.start()
    pl.semaphore_wait(barrier, ny + nz - 2)
    tables[0].wait()
    x_forward(0, 0, pairs)
    x_prefetch(0)
    for jj in range(1, HALF_X_CHUNKS):
        for o in x_offsets:
            xf(jj, o).start()
    for table in tables[1:]:
        table.wait()

    def step(t, carry):
        @pl.when(t < nj)
        def _():
            xf_wait(t)
            y_forward(t)
            for o in y_offsets:
                yf(t, o).start()

        @pl.when((t >= 1) & (t < nj + 1))
        def _():
            j = t - 1
            yf_wait(j)
            for c in range(2):
                g_copy(c, j).wait()
            z_solve(j)
            for o in y_offsets:
                yi(j, o).start()

            @pl.when(j + 2 < nj)
            def _():
                for c in range(2):
                    g_copy(c, j + 2).start()

        @pl.when(t >= 2)
        def _():
            j = t - 2
            yi_wait(j)
            y_inverse(j)
            for o in x_offsets:
                xi(j, o).start()
            own(bbuf, ebuf, j, py, xrow)

        @pl.when(t < 4)
        def _():
            x_forward(1, t * quarter, (t + 1) * quarter)

            @pl.when(t < 3)
            def _():
                x_prefetch((t + 1) * quarter)

        @pl.when(t == 3)
        def _():
            def send(jj, c):
                for o in x_offsets:
                    xf(jj, o).start()
                return c

            lax.fori_loop(HALF_X_CHUNKS, nj, send, 0)

        @pl.when(t == nj - 4)
        def _():
            for jj in range(HALF_X_CHUNKS):
                xi_wait(jj)

        @pl.when((t >= nj - 4) & (t < nj))
        def _():
            def body(k, c):
                pair = (t - (nj - 4)) * quarter + k
                even[pair] = x_inverse(ebuf, wxi, 0, pair, ny, crow, xrow)
                return c

            lax.fori_loop(0, quarter, body, 0)

        return carry

    lax.fori_loop(0, nj + 2, step, 0)
    for jj in range(HALF_X_CHUNKS, nj):
        xi_wait(jj)


def x_inverse(ebuf, wxi, p, pair, ny, crow, xrow):
    tiles = [ebuf[pl.ds(pl.multiple_of((p * HALF_X_CHUNKS + jj) * crow + src * xrow + pair * 8, 8), 8), :]
             for jj in range(HALF_X_CHUNKS) for src in range(ny)]
    first, second = swap_rows(jnp.concatenate(tiles[::2], axis=0), jnp.concatenate(tiles[1::2], axis=0))
    lines = [first.reshape(-1, LANES), second.reshape(-1, LANES)]
    return dot(jnp.concatenate(lines, axis=1), wxi[p], ((0,), (0,)))


def finish(ny, n, nf, ebuf, even, hat_re, hat_im, wxi, phi_re, phi_im, out_re, out_im, stage, p_sem, h_sem):
    half = n // 2
    yl = n // ny
    nj, pairs = 2 * HALF_X_CHUNKS, yl // 2
    crow = ebuf.shape[0] // nj
    xrow = crow // ny
    zl = phi_re.shape[2]
    phi = (phi_re, phi_im)
    hats = [pltpu.make_async_copy(a, b, h_sem.at[c]) for c, (a, b) in enumerate(((hat_re, out_re), (hat_im, out_im)))]
    for h in hats:
        h.start()

    def phi_copy(c, pair):
        slot = lax.rem(pair, 2)
        return pltpu.make_async_copy(stage.at[slot, c], phi[c].at[:, pl.ds(2 * pair, 2)], p_sem.at[slot, c])

    def body(pair, carry):
        slot = lax.rem(pair, 2)
        e, o = even[pair], x_inverse(ebuf, wxi, 1, pair, ny, crow, xrow)

        @pl.when(pair >= 2)
        def _():
            for c in range(2):
                phi_copy(c, pair - 2).wait()

        for c in range(2):
            ec, oc = e[:, c * half:(c + 1) * half], o[:, c * half:(c + 1) * half]
            out = jnp.concatenate([ec + oc, ec - oc], axis=1).reshape(2, nf, zl, n)
            stage[slot, c] = jnp.swapaxes(out, 0, 1)
            phi_copy(c, pair).start()
        return carry

    lax.fori_loop(0, pairs, body, 0)
    for pair in (pairs - 2, pairs - 1):
        for c in range(2):
            phi_copy(c, pair).wait()
    for h in hats:
        h.wait()


def solution(mesh):
    ny, nz = mesh.shape["py"], mesh.shape["pz"]

    def local_solve(rho_re, rho_im, g_re, g_im):
        nf, n, yl, zl = rho_re.shape
        kl, ml = g_re.shape[:2]
        kc = kl // HALF_X_CHUNKS // 2
        nj = 2 * HALF_X_CHUNKS
        rows = nj * ny * yl * 2 * kc
        tables = [jnp.asarray(w) for w in dft_tables(n, ny, nz)]
        space = jax.ShapeDtypeStruct((nf, yl, zl, n), jnp.float32)
        wave_shape = (nf, kl // 2, 2, ml, n)
        wave = jax.ShapeDtypeStruct(wave_shape, jnp.float32)
        dma = pltpu.SemaphoreType.DMA
        buf = pltpu.VMEM((rows, LANES), jnp.float32)
        vmem = pl.BlockSpec(memory_space=pltpu.VMEM)
        hbm = pl.BlockSpec(memory_space=pl.ANY)
        inner = pl.pallas_call(
            functools.partial(kernel, ny, nz, n, nf),
            out_shape=(pltpu.VMEM((rows, LANES), jnp.float32), pltpu.VMEM((yl // 2, 2 * nf * zl, n), jnp.float32),
                       pltpu.VMEM(wave_shape, jnp.float32), pltpu.VMEM(wave_shape, jnp.float32)),
            in_specs=[hbm] * 10,
            out_specs=[vmem] * 4,
            scratch_shapes=[
                buf, buf, buf, buf,
                pltpu.VMEM((SLOTS, 2, nf, 2, zl, n), jnp.float32),
                pltpu.VMEM((2, 2, kc, ml, n), jnp.float32),
                *[pltpu.VMEM(t.shape, jnp.float32) for t in tables],
                *[dma((nj,)) for _ in range(8)],
                dma((len(tables),)), dma((SLOTS, 2)), dma((2, 2)),
            ],
            compiler_params=pltpu.CompilerParams(
                collective_id=0, has_side_effects=True, vmem_limit_bytes=INNER_VMEM),
            name="spectral",
        )(jnp.transpose(rho_re, (0, 2, 3, 1)), jnp.transpose(rho_im, (0, 2, 3, 1)),
          g_re.reshape(kl // 2, 2, ml, n), g_im.reshape(kl // 2, 2, ml, n), *tables)
        outs = pl.pallas_call(
            functools.partial(finish, ny, n, nf),
            out_shape=(space, space, wave, wave),
            in_specs=[vmem] * 5,
            out_specs=[hbm] * 4,
            scratch_shapes=[pltpu.VMEM((2, 2, nf, 2, zl, n), jnp.float32), dma((2, 2)), dma((2,))],
            compiler_params=pltpu.CompilerParams(vmem_limit_bytes=16 << 20),
            name="finish",
        )(*inner, tables[5])
        phi = [jnp.transpose(v, (0, 3, 1, 2)) for v in outs[:2]]
        return (*phi, *(v.reshape(nf, kl, ml, n) for v in outs[2:]))

    space_layout = P("dp", None, "py", "pz")
    wave_layout = P("dp", "py", "pz", None)
    green_layout = P("py", "pz", None)
    return jax.shard_map(local_solve, mesh=mesh,
                         in_specs=(space_layout, space_layout, green_layout, green_layout),
                         out_specs=(space_layout, space_layout, wave_layout, wave_layout),
                         check_vma=False)
```

```python
import functools

import jax
import jax.numpy as jnp
import numpy as np
from jax import lax
from jax.experimental import pallas as pl
from jax.experimental.pallas import tpu as pltpu
from jax.sharding import PartitionSpec as P

MESH = pl.DeviceIdType.MESH
HALF_X_CHUNKS = 8
SLOTS = 3
GROUP = 2
OUT_SLOTS = 8
LANES = 128
INNER_VMEM = 42 << 20


def real_form(matrix):
    return np.block([[matrix.real, -matrix.imag], [matrix.imag, matrix.real]])


def dft_tables(n, ny, nz):
    half = n // 2
    scale = 1.0 / np.sqrt(n)
    low, full = np.arange(half), np.arange(n)
    dft = lambda k, j, sign: scale * np.exp(sign * 2j * np.pi * ((k[:, None] * j[None, :]) % n) / n)
    per = n // ny // HALF_X_CHUNKS // 2
    order = np.arange(half).reshape(ny, HALF_X_CHUNKS, per).transpose(1, 0, 2)
    rows = np.stack([order, order + half], axis=2).reshape(-1)
    wx = np.stack([real_form(dft(2 * low + p, low, -1))[rows] for p in range(2)])
    wy = np.stack([real_form(dft(2 * low + p, low, -1)) for p in range(2)])
    wyi = np.stack([real_form(dft(low, 2 * low + p, 1)) for p in range(2)])
    lz = n // nz
    zrows = np.arange(n).reshape(nz, lz)
    zrows = np.stack([zrows, zrows + n], axis=1).reshape(-1)
    wz = real_form(dft(full, full, -1)).T[zrows]
    return [np.asarray(w, np.float32) for w in (wx, wy, wz, wyi)]


def dot(a, b, dims=((1,), (0,))):
    return lax.dot_general(a, b, (dims, ((), ())), precision=lax.Precision.HIGHEST,
                           preferred_element_type=jnp.float32)


def swap_rows(first, second):
    a, b = first.reshape(-1, 8, LANES), second.reshape(-1, 8, LANES)
    upper = lax.broadcasted_iota(jnp.int32, a.shape, 1) < 4
    return jnp.where(upper, a, pltpu.roll(b, 4, 1)), jnp.where(upper, pltpu.roll(a, 4, 1), b)


def kernel(ny, nz, n, nf,
           rho_re, rho_im, g_re, g_im, wx_h, wy_h, wz_h, wyi_h,
           ebuf, even, hat_re, hat_im,
           abuf, bbuf, cbuf, dbuf, stage, gbuf, wx, wy, wz, wyi,
           xs, xr, ys, yr, yis, yir, xis, xir, w_sem, in_sem, g_sem):
    py, pz = lax.axis_index("py"), lax.axis_index("pz")
    half = n // 2
    yl, zl = n // ny, n // nz
    kc = n // ny // HALF_X_CHUNKS // 2
    nj = 2 * HALF_X_CHUNKS
    xrow, yrow = yl * 2 * kc, 2 * kc * zl
    crow = ny * xrow
    pairs = yl // 2
    quarter = pairs // 4
    groups = pairs // GROUP
    piece = groups // 4
    rho, gg, hat = (rho_re, rho_im), (g_re, g_im), (hat_re, hat_im)
    x_offsets = (4, 3, 5, 2, 6, 1, 7) if ny == 8 else tuple(range(1, ny))
    y_offsets = (2, 1, 3) if nz == 4 else tuple(range(1, nz))

    barrier = pltpu.get_barrier_semaphore()
    tables = [pltpu.make_async_copy(h, v, w_sem.at[i]) for i, (h, v) in enumerate(
        ((wx_h, wx), (wy_h, wy), (wz_h, wz), (wyi_h, wyi)))]

    def rho_copy(c, group):
        slot = lax.rem(group, SLOTS)
        return pltpu.make_async_copy(rho[c].at[:, pl.ds(2 * GROUP * group, 2 * GROUP)], stage.at[slot, c],
                                     in_sem.at[slot, c])

    def g_copy(c, j):
        p, jj, slot = j // HALF_X_CHUNKS, lax.rem(j, HALF_X_CHUNKS), lax.rem(j, 2)
        return pltpu.make_async_copy(gg[c].at[pl.ds(kc * jj, kc), p], gbuf.at[slot, c], g_sem.at[slot, c])

    def x_copy(src, dst, ss, rs, j, o, first=0, count=None):
        to = lax.rem(py + o, ny)
        rows = xrow if count is None else count
        return pltpu.make_async_remote_copy(
            src.at[pl.ds(pl.multiple_of(j * crow + to * xrow + first, 8), rows)],
            dst.at[pl.ds(pl.multiple_of(j * crow + py * xrow + first, 8), rows)],
            ss.at[j], rs.at[j], device_id={"py": to}, device_id_type=MESH)

    def y_copy(src, dst, ss, rs, j, o):
        to = lax.rem(pz + o, nz)
        return pltpu.make_async_remote_copy(
            src.at[pl.ds(pl.multiple_of(j * crow + to * yrow, 8), yrow)],
            dst.at[pl.ds(pl.multiple_of(j * crow + pz * yrow, 8), yrow)],
            ss.at[j], rs.at[j], device_id={"pz": to}, device_id_type=MESH)

    def await_all(src, dst, ss, rs, j, axis, me, size, rows):
        at = pl.ds(pl.multiple_of(j * crow, 8), rows)
        pltpu.make_async_remote_copy(src.at[at], dst.at[at], ss.at[j], rs.at[j],
                                     device_id={axis: lax.rem(me + 1, size)}, device_id_type=MESH).wait()

    def own(src, dst, j, mine, rows):
        at = pl.ds(pl.multiple_of(j * crow + mine * rows, 8), rows)
        dst[at, :] = src[at, :]

    xf = functools.partial(x_copy, abuf, bbuf, xs, xr)
    yf = functools.partial(y_copy, abuf, cbuf, ys, yr)
    yi = functools.partial(y_copy, cbuf, dbuf, yis, yir)
    xi = functools.partial(x_copy, bbuf, ebuf, xis, xir)
    xf_wait = lambda j: await_all(abuf, bbuf, xs, xr, j, "py", py, ny, (ny - 1) * xrow)
    yf_wait = lambda j: await_all(abuf, cbuf, ys, yr, j, "pz", pz, nz, (nz - 1) * yrow)
    yi_wait = lambda j: await_all(cbuf, dbuf, yis, yir, j, "pz", pz, nz, (nz - 1) * yrow)
    xi_wait = lambda j: await_all(bbuf, ebuf, xis, xir, j, "py", py, ny, (ny - 1) * xrow)

    def x_prefetch(first):
        for k in range(SLOTS - 1):
            for c in range(2):
                rho_copy(c, first + k).start()

    def x_forward(p, first, stop):
        def body(group, carry):
            @pl.when(group + SLOTS - 1 < stop)
            def _():
                for c in range(2):
                    rho_copy(c, group + SLOTS - 1).start()

            for c in range(2):
                rho_copy(c, group).wait()
            slot = lax.rem(group, SLOTS)
            for u in range(GROUP):
                folded = []
                for c in range(2):
                    lines = stage[slot, c, :, 2 * u:2 * u + 2]
                    low, high = lines[..., :half], lines[..., half:]
                    both = low - high if p else low + high
                    folded.append(jnp.swapaxes(both, 0, 1).reshape(2 * nf * zl, half))
                out = dot(wx[p], jnp.concatenate(folded, axis=1), ((1,), (1,)))
                blocks = swap_rows(out[:, :LANES], out[:, LANES:])
                for jj in range(HALF_X_CHUNKS):
                    for to in range(ny):
                        r = jj * ny + to
                        at = (p * HALF_X_CHUNKS + jj) * crow + to * xrow + (group * GROUP + u) * 8
                        abuf[pl.ds(pl.multiple_of(at, 8), 8), :] = blocks[r % 2][r // 2]
            if p == 0:
                @pl.when(group == first)
                def _():
                    pl.semaphore_wait(barrier, ny + nz - 2)

                for o in x_offsets:
                    xf(0, o, group * GROUP * 8, GROUP * 8).start()
            return carry

        lax.fori_loop(first, stop, body, 0)

    def y_forward(j):
        own(abuf, bbuf, j, py, xrow)
        base = j * crow
        parts = []
        for c in range(2):
            parts.append(jnp.concatenate(
                [bbuf[pl.ds(base + c * kc + i, n, stride=2 * kc), :] for i in range(2)], axis=1))
        for p in range(2):
            folded = jnp.concatenate([v[:half] - v[half:] if p else v[:half] + v[half:] for v in parts], axis=0)
            out = dot(wy[p], folded)
            for c in range(2):
                for to in range(nz):
                    for k in range(2):
                        at = base + to * yrow + (c * kc + k) * zl + p
                        abuf[pl.ds(at, zl // 2, stride=2), :] = out[
                            c * half + to * zl // 2:c * half + (to + 1) * zl // 2, k * LANES:(k + 1) * LANES]

    def z_solve(j):
        own(abuf, cbuf, j, pz, yrow)
        base, slot = j * crow, lax.rem(j, 2)
        p, jj = j // HALF_X_CHUNKS, lax.rem(j, HALF_X_CHUNKS)
        rows = kc * zl
        left = lax.broadcasted_iota(jnp.int32, (rows, LANES), 1) < zl
        swap = lambda v: pltpu.roll(v, zl, 1)
        lines = ([], [])
        for b in range(nz):
            at = base + b * yrow
            re = cbuf[pl.ds(pl.multiple_of(at, 8), rows), :]
            im = cbuf[pl.ds(pl.multiple_of(at + rows, 8), rows), :]
            lines[0].append(jnp.where(left, re, swap(im)))
            lines[1].append(jnp.where(left, swap(re), im))
        both = jnp.concatenate([jnp.concatenate(v, axis=1) for v in lines], axis=0)
        spec = dot(both, wz[...])
        gr = gbuf[slot, 0].reshape(rows, n)
        gi = gbuf[slot, 1].reshape(rows, n)
        scaled = []
        for f in range(nf):
            sr, si = spec[f * rows:(f + 1) * rows, :n], spec[f * rows:(f + 1) * rows, n:]
            hr, hi = sr * gr - si * gi, sr * gi + si * gr
            hat_re[f, pl.ds(kc * jj, kc), p] = hr.reshape(kc, zl, n)
            hat_im[f, pl.ds(kc * jj, kc), p] = hi.reshape(kc, zl, n)
            scaled.append(jnp.concatenate([hr, hi], axis=1))
        back = dot(jnp.concatenate(scaled, axis=0), wz[...], ((1,), (1,)))
        for b in range(nz):
            first, second = (back[f * rows:(f + 1) * rows, b * LANES:(b + 1) * LANES] for f in range(2))
            at = base + b * yrow
            cbuf[pl.ds(pl.multiple_of(at, 8), rows), :] = jnp.where(left, first, swap(second))
            cbuf[pl.ds(pl.multiple_of(at + rows, 8), rows), :] = jnp.where(left, swap(first), second)

    def y_inverse(j):
        own(cbuf, dbuf, j, pz, yrow)
        base = j * crow
        halves = []
        for p in range(2):
            lines = []
            for k in range(2):
                lines.append(jnp.concatenate(
                    [dbuf[pl.ds(base + src * yrow + (c * kc + k) * zl + p, zl // 2, stride=2), :]
                     for c in range(2) for src in range(nz)], axis=0))
            halves.append(dot(wyi[p], jnp.concatenate(lines, axis=1)))
        for s, out in enumerate((halves[0] + halves[1], halves[0] - halves[1])):
            for c in range(2):
                for k in range(2):
                    at = base + s * (ny // 2) * xrow + c * kc + k
                    bbuf[pl.ds(at, half, stride=2 * kc), :] = out[
                        c * half:(c + 1) * half, k * LANES:(k + 1) * LANES]

    x_prefetch(0)
    tables[0].start()
    for o in range(1, ny):
        pl.semaphore_signal(barrier, inc=1, device_id={"py": lax.rem(py + o, ny)}, device_id_type=MESH)
    for o in range(1, nz):
        pl.semaphore_signal(barrier, inc=1, device_id={"pz": lax.rem(pz + o, nz)}, device_id_type=MESH)
    tables[0].wait()
    x_forward(0, 0, groups)
    for c in range(2):
        g_copy(c, 0).start()
        g_copy(c, 1).start()
    for table in tables[1:]:
        table.start()
    x_prefetch(0)
    for jj in range(1, HALF_X_CHUNKS):
        for o in x_offsets:
            xf(jj, o).start()
    for table in tables[1:]:
        table.wait()

    def step(t, carry):
        @pl.when(t < nj)
        def _():
            xf_wait(t)
            y_forward(t)
            for o in y_offsets:
                yf(t, o).start()

        @pl.when((t >= 1) & (t < nj + 1))
        def _():
            j = t - 1
            yf_wait(j)
            for c in range(2):
                g_copy(c, j).wait()
            z_solve(j)
            for o in y_offsets:
                yi(j, o).start()

            @pl.when(j + 2 < nj)
            def _():
                for c in range(2):
                    g_copy(c, j + 2).start()

        @pl.when(t >= 2)
        def _():
            j = t - 2
            yi_wait(j)
            y_inverse(j)
            for o in x_offsets:
                xi(j, o).start()
            own(bbuf, ebuf, j, py, xrow)

        @pl.when(t < 4)
        def _():
            x_forward(1, t * piece, (t + 1) * piece)

            @pl.when(t < 3)
            def _():
                x_prefetch((t + 1) * piece)

        @pl.when(t == 3)
        def _():
            def send(jj, c):
                for o in x_offsets:
                    xf(jj, o).start()
                return c

            lax.fori_loop(HALF_X_CHUNKS, nj, send, 0)

        @pl.when(t == nj - 4)
        def _():
            for jj in range(HALF_X_CHUNKS):
                xi_wait(jj)

        @pl.when((t >= nj - 4) & (t < nj))
        def _():
            def body(k, c):
                pair = (t - (nj - 4)) * quarter + k
                even[pair] = x_inverse(ebuf, wx, 0, pair, ny, crow, xrow)
                return c

            lax.fori_loop(0, quarter, body, 0)

        return carry

    lax.fori_loop(0, nj + 2, step, 0)
    for jj in range(HALF_X_CHUNKS, nj):
        xi_wait(jj)


def x_inverse(ebuf, wx, p, pair, ny, crow, xrow):
    tiles = [ebuf[pl.ds(pl.multiple_of((p * HALF_X_CHUNKS + jj) * crow + src * xrow + pair * 8, 8), 8), :]
             for jj in range(HALF_X_CHUNKS) for src in range(ny)]
    first, second = swap_rows(jnp.concatenate(tiles[::2], axis=0), jnp.concatenate(tiles[1::2], axis=0))
    lines = [first.reshape(-1, LANES), second.reshape(-1, LANES)]
    return dot(jnp.concatenate(lines, axis=1), wx[p], ((0,), (0,)))


def finish(ny, n, nf, ebuf, even, hat_re, hat_im, wx, phi_re, phi_im, out_re, out_im, stage, p_sem, h_sem):
    half = n // 2
    yl = n // ny
    nj, pairs = 2 * HALF_X_CHUNKS, yl // 2
    crow = ebuf.shape[0] // nj
    xrow = crow // ny
    zl = phi_re.shape[2]
    phi = (phi_re, phi_im)
    hats = [pltpu.make_async_copy(a, b, h_sem.at[c]) for c, (a, b) in enumerate(((hat_re, out_re), (hat_im, out_im)))]
    for h in hats:
        h.start()

    def phi_copy(c, pair):
        slot = lax.rem(pair, OUT_SLOTS)
        return pltpu.make_async_copy(stage.at[slot, c], phi[c].at[:, pl.ds(2 * pair, 2)], p_sem.at[slot, c])

    def body(group, carry):
        @pl.when(group * GROUP >= OUT_SLOTS)
        def _():
            for u in range(GROUP):
                for c in range(2):
                    phi_copy(c, group * GROUP + u - OUT_SLOTS).wait()

        for u in range(GROUP):
            pair = group * GROUP + u
            slot = lax.rem(pair, OUT_SLOTS)
            e, o = even[pair], x_inverse(ebuf, wx, 1, pair, ny, crow, xrow)
            for c in range(2):
                ec, oc = e[:, c * half:(c + 1) * half], o[:, c * half:(c + 1) * half]
                out = jnp.concatenate([ec + oc, ec - oc], axis=1).reshape(2, nf, zl, n)
                stage[slot, c] = jnp.swapaxes(out, 0, 1)
        for u in range(GROUP):
            for c in range(2):
                phi_copy(c, group * GROUP + u).start()
        return carry

    lax.fori_loop(0, pairs // GROUP, body, 0)
    for pair in range(pairs - OUT_SLOTS, pairs):
        for c in range(2):
            phi_copy(c, pair).wait()
    for h in hats:
        h.wait()


def solution(mesh):
    ny, nz = mesh.shape["py"], mesh.shape["pz"]

    def local_solve(rho_re, rho_im, g_re, g_im):
        nf, n, yl, zl = rho_re.shape
        kl, ml = g_re.shape[:2]
        kc = kl // HALF_X_CHUNKS // 2
        nj = 2 * HALF_X_CHUNKS
        rows = nj * ny * yl * 2 * kc
        tables = [jnp.asarray(w) for w in dft_tables(n, ny, nz)]
        space = jax.ShapeDtypeStruct((nf, yl, zl, n), jnp.float32)
        wave_shape = (nf, kl // 2, 2, ml, n)
        wave = jax.ShapeDtypeStruct(wave_shape, jnp.float32)
        dma = pltpu.SemaphoreType.DMA
        buf = pltpu.VMEM((rows, LANES), jnp.float32)
        vmem = pl.BlockSpec(memory_space=pltpu.VMEM)
        hbm = pl.BlockSpec(memory_space=pl.ANY)
        inner = pl.pallas_call(
            functools.partial(kernel, ny, nz, n, nf),
            out_shape=(pltpu.VMEM((rows, LANES), jnp.float32), pltpu.VMEM((yl // 2, 2 * nf * zl, n), jnp.float32),
                       pltpu.VMEM(wave_shape, jnp.float32), pltpu.VMEM(wave_shape, jnp.float32)),
            in_specs=[hbm] * 8,
            out_specs=[vmem] * 4,
            scratch_shapes=[
                buf, buf, buf, buf,
                pltpu.VMEM((SLOTS, 2, nf, 2 * GROUP, zl, n), jnp.float32),
                pltpu.VMEM((2, 2, kc, ml, n), jnp.float32),
                *[pltpu.VMEM(t.shape, jnp.float32) for t in tables],
                *[dma((nj,)) for _ in range(8)],
                dma((len(tables),)), dma((SLOTS, 2)), dma((2, 2)),
            ],
            compiler_params=pltpu.CompilerParams(
                collective_id=0, has_side_effects=True, vmem_limit_bytes=INNER_VMEM),
            name="spectral",
        )(jnp.transpose(rho_re, (0, 2, 3, 1)), jnp.transpose(rho_im, (0, 2, 3, 1)),
          g_re.reshape(kl // 2, 2, ml, n), g_im.reshape(kl // 2, 2, ml, n), *tables)
        outs = pl.pallas_call(
            functools.partial(finish, ny, n, nf),
            out_shape=(space, space, wave, wave),
            in_specs=[vmem] * 5,
            out_specs=[hbm] * 4,
            scratch_shapes=[pltpu.VMEM((OUT_SLOTS, 2, nf, 2, zl, n), jnp.float32), dma((OUT_SLOTS, 2)), dma((2,))],
            compiler_params=pltpu.CompilerParams(vmem_limit_bytes=16 << 20),
            name="finish",
        )(*inner, tables[0])
        phi = [jnp.transpose(v, (0, 3, 1, 2)) for v in outs[:2]]
        return (*phi, *(v.reshape(nf, kl, ml, n) for v in outs[2:]))

    space_layout = P("dp", None, "py", "pz")
    wave_layout = P("dp", "py", "pz", None)
    green_layout = P("py", "pz", None)
    return jax.shard_map(local_solve, mesh=mesh,
                         in_specs=(space_layout, space_layout, green_layout, green_layout),
                         out_specs=(space_layout, space_layout, wave_layout, wave_layout),
                         check_vma=False)
```

```python
import functools

import jax
import jax.numpy as jnp
import numpy as np
from jax import lax
from jax.experimental import pallas as pl
from jax.experimental.pallas import tpu as pltpu
from jax.sharding import PartitionSpec as P

MESH = pl.DeviceIdType.MESH
HALF_X_CHUNKS = 8
SLOTS = 3
GROUP = 2
OUT_SLOTS = 4
LANES = 128
INNER_VMEM = 42 << 20


def real_form(matrix):
    return np.block([[matrix.real, -matrix.imag], [matrix.imag, matrix.real]])


def dft_tables(n, ny, nz):
    half = n // 2
    scale = 1.0 / np.sqrt(n)
    low, full = np.arange(half), np.arange(n)
    dft = lambda k, j, sign: scale * np.exp(sign * 2j * np.pi * ((k[:, None] * j[None, :]) % n) / n)
    per = n // ny // HALF_X_CHUNKS // 2
    order = np.arange(half).reshape(ny, HALF_X_CHUNKS, per).transpose(1, 0, 2)
    rows = np.stack([order, order + half], axis=3).reshape(-1)
    wx = np.stack([real_form(dft(2 * low + p, low, -1))[rows] for p in range(2)])
    wy = np.stack([real_form(dft(2 * low + p, low, -1)) for p in range(2)])
    wyi = np.stack([real_form(dft(low, 2 * low + p, 1)) for p in range(2)])
    lz = n // nz
    zrows = np.arange(n).reshape(nz, lz)
    zrows = np.stack([zrows, zrows + n], axis=1).reshape(-1)
    wz = real_form(dft(full, full, -1)).T[zrows]
    return [np.asarray(w, np.float32) for w in (wx, wy, wz, wyi)]


def dot(a, b, dims=((1,), (0,))):
    return lax.dot_general(a, b, (dims, ((), ())), precision=lax.Precision.HIGHEST,
                           preferred_element_type=jnp.float32)


def swap_rows(first, second):
    a, b = first.reshape(-1, 8, LANES), second.reshape(-1, 8, LANES)
    upper = lax.broadcasted_iota(jnp.int32, a.shape, 1) < 4
    return jnp.where(upper, a, pltpu.roll(b, 4, 1)), jnp.where(upper, pltpu.roll(a, 4, 1), b)


def swap_pairs(a, b):
    kept = lax.broadcasted_iota(jnp.int32, a.shape, 1) & 2 == 0
    return jnp.where(kept, a, pltpu.roll(b, 2, 1)), jnp.where(kept, pltpu.roll(a, 6, 1), b)


def kernel(ny, nz, n, nf,
           rho_re, rho_im, g_re, g_im, wx_h, wy_h, wz_h, wyi_h,
           ebuf, even, hat_re, hat_im,
           abuf, bbuf, cbuf, dbuf, stage, gbuf, wx, wy, wz, wyi,
           xs, xr, ys, yr, yis, yir, xis, xir, w_sem, in_sem, g_sem):
    py, pz = lax.axis_index("py"), lax.axis_index("pz")
    half = n // 2
    yl, zl = n // ny, n // nz
    kc = n // ny // HALF_X_CHUNKS // 2
    nj = 2 * HALF_X_CHUNKS
    xrow, yrow = yl * 2 * kc, 2 * kc * zl
    crow = ny * xrow
    pairs = yl // 2
    groups = pairs // GROUP
    piece = groups // 4
    sends = ((0, groups // 2), (groups // 2, piece), (groups - piece, piece // 2), (groups - piece // 2, piece // 2))
    rho, gg, hat = (rho_re, rho_im), (g_re, g_im), (hat_re, hat_im)
    x_offsets = (4, 3, 5, 2, 6, 1, 7) if ny == 8 else tuple(range(1, ny))
    y_offsets = (2, 1, 3) if nz == 4 else tuple(range(1, nz))

    barrier = pltpu.get_barrier_semaphore()
    tables = [pltpu.make_async_copy(h, v, w_sem.at[i]) for i, (h, v) in enumerate(
        ((wx_h, wx), (wy_h, wy), (wz_h, wz), (wyi_h, wyi)))]

    def rho_copy(c, group):
        slot = lax.rem(group, SLOTS)
        return pltpu.make_async_copy(rho[c].at[:, pl.ds(2 * GROUP * group, 2 * GROUP)], stage.at[slot, c],
                                     in_sem.at[slot, c])

    def g_copy(c, j):
        p, jj, slot = j // HALF_X_CHUNKS, lax.rem(j, HALF_X_CHUNKS), lax.rem(j, 2)
        return pltpu.make_async_copy(gg[c].at[pl.ds(kc * jj, kc), p], gbuf.at[slot, c], g_sem.at[slot, c])

    def x_copy(src, dst, ss, rs, j, o, first=0, count=None, *half_of):
        to = lax.rem(py + o, ny)
        rows = xrow if count is None else count
        return pltpu.make_async_remote_copy(
            src.at[pl.ds(pl.multiple_of(j * crow + to * xrow + first, 8), rows)],
            dst.at[pl.ds(pl.multiple_of(j * crow + py * xrow + first, 8), rows)],
            ss.at[j, *half_of], rs.at[j, *half_of], device_id={"py": to}, device_id_type=MESH)

    def y_copy(src, dst, ss, rs, j, o, first=0, count=None, *half_of):
        to = lax.rem(pz + o, nz)
        rows = yrow if count is None else count
        return pltpu.make_async_remote_copy(
            src.at[pl.ds(pl.multiple_of(j * crow + to * yrow + first, 8), rows)],
            dst.at[pl.ds(pl.multiple_of(j * crow + pz * yrow + first, 8), rows)],
            ss.at[j, *half_of], rs.at[j, *half_of], device_id={"pz": to}, device_id_type=MESH)

    def await_all(src, dst, ss, rs, axis, me, size, rows, *of):
        at = pl.ds(pl.multiple_of(of[0] * crow, 8), rows)
        pltpu.make_async_remote_copy(src.at[at], dst.at[at], ss.at[*of], rs.at[*of],
                                     device_id={axis: lax.rem(me + 1, size)}, device_id_type=MESH).wait()

    def own(src, dst, j, mine, rows):
        at = pl.ds(pl.multiple_of(j * crow + mine * rows, 8), rows)
        dst[at, :] = src[at, :]

    xf = functools.partial(x_copy, abuf, bbuf, xs, xr)
    yf = functools.partial(y_copy, abuf, cbuf, ys, yr)
    yi = functools.partial(y_copy, cbuf, dbuf, yis, yir)
    xi = functools.partial(x_copy, bbuf, ebuf, xis, xir)
    xf_wait = functools.partial(await_all, abuf, bbuf, xs, xr, "py", py, ny, (ny - 1) * xrow)
    yf_wait = functools.partial(await_all, abuf, cbuf, ys, yr, "pz", pz, nz, (nz - 1) * yrow)
    yi_wait = functools.partial(await_all, cbuf, dbuf, yis, yir, "pz", pz, nz, (nz - 1) * yrow // 2)
    xi_wait = functools.partial(await_all, bbuf, ebuf, xis, xir, "py", py, ny, (ny - 1) * xrow // 2)

    def x_prefetch(first):
        for k in range(SLOTS - 1):
            for c in range(2):
                rho_copy(c, first + k).start()

    def x_forward(p, first, stop):
        def body(group, carry):
            @pl.when(group + SLOTS - 1 < stop)
            def _():
                for c in range(2):
                    rho_copy(c, group + SLOTS - 1).start()

            for c in range(2):
                rho_copy(c, group).wait()
            slot = lax.rem(group, SLOTS)
            folded = []
            for c in range(2):
                lines = stage[slot, c]
                low, high = lines[..., :half], lines[..., half:]
                both = low - high if p else low + high
                folded.append(jnp.swapaxes(both, 0, 1).reshape(2 * GROUP * nf * zl, half))
            out = dot(wx[p], jnp.concatenate(folded, axis=1), ((1,), (1,)))
            for u in range(GROUP):
                blocks = swap_rows(out[:, 2 * u * LANES:(2 * u + 1) * LANES],
                                   out[:, (2 * u + 1) * LANES:(2 * u + 2) * LANES])
                for jj in range(HALF_X_CHUNKS):
                    for to in range(ny):
                        r = jj * ny + to
                        at = (p * HALF_X_CHUNKS + jj) * crow + to * xrow + (group * GROUP + u) * 8
                        abuf[pl.ds(pl.multiple_of(at, 8), 8), :] = blocks[r % 2][r // 2]
            if p == 0:
                for start, count in sends:
                    @pl.when(group == start + count - 1)
                    def _():
                        if start == 0:
                            pl.semaphore_wait(barrier, ny + nz - 2)
                        for o in x_offsets:
                            xf(0, o, start * GROUP * 8, count * GROUP * 8).start()
            return carry

        lax.fori_loop(first, stop, body, 0)

    def y_forward(j):
        own(abuf, bbuf, j, py, xrow)
        base = j * crow
        parts = []
        for c in range(2):
            parts.append(jnp.concatenate(
                [bbuf[pl.ds(base + 2 * i + c, n, stride=2 * kc), :] for i in range(2)], axis=1))
        for p in range(2):
            folded = jnp.concatenate([v[:half] - v[half:] if p else v[:half] + v[half:] for v in parts], axis=0)
            out = dot(wy[p], folded)
            for c in range(2):
                for to in range(nz):
                    for k in range(2):
                        at = base + to * yrow + (c * kc + k) * zl + p
                        abuf[pl.ds(at, zl // 2, stride=2), :] = out[
                            c * half + to * zl // 2:c * half + (to + 1) * zl // 2, k * LANES:(k + 1) * LANES]

    def z_solve(j):
        own(abuf, cbuf, j, pz, yrow)
        base, slot = j * crow, lax.rem(j, 2)
        p, jj = j // HALF_X_CHUNKS, lax.rem(j, HALF_X_CHUNKS)
        rows = kc * zl
        left = lax.broadcasted_iota(jnp.int32, (rows, LANES), 1) < zl
        swap = lambda v: pltpu.roll(v, zl, 1)
        lines = ([], [])
        for b in range(nz):
            at = base + b * yrow
            re = cbuf[pl.ds(pl.multiple_of(at, 8), rows), :]
            im = cbuf[pl.ds(pl.multiple_of(at + rows, 8), rows), :]
            lines[0].append(jnp.where(left, re, swap(im)))
            lines[1].append(jnp.where(left, swap(re), im))
        both = jnp.concatenate([jnp.concatenate(v, axis=1) for v in lines], axis=0)
        spec = dot(both, wz[...])
        gr = gbuf[slot, 0].reshape(rows, n)
        gi = gbuf[slot, 1].reshape(rows, n)
        scaled = []
        for f in range(nf):
            sr, si = spec[f * rows:(f + 1) * rows, :n], spec[f * rows:(f + 1) * rows, n:]
            hr, hi = sr * gr - si * gi, sr * gi + si * gr
            hat_re[f, pl.ds(kc * jj, kc), p] = hr.reshape(kc, zl, n)
            hat_im[f, pl.ds(kc * jj, kc), p] = hi.reshape(kc, zl, n)
            scaled.append(jnp.concatenate([hr, hi], axis=1))
        back = dot(jnp.concatenate(scaled, axis=0), wz[...], ((1,), (1,)))
        for b in range(nz):
            first, second = (back[f * rows:(f + 1) * rows, b * LANES:(b + 1) * LANES] for f in range(2))
            at = base + b * yrow
            cbuf[pl.ds(pl.multiple_of(at, 8), rows), :] = jnp.where(left, first, swap(second))
            cbuf[pl.ds(pl.multiple_of(at + rows, 8), rows), :] = jnp.where(left, swap(first), second)

    def y_inverse(j, i):
        base = j * crow
        halves = []
        for p in range(2):
            lines = jnp.concatenate(
                [dbuf[pl.ds(base + src * yrow + (c * kc + i) * zl + p, zl // 2, stride=2), :]
                 for c in range(2) for src in range(nz)], axis=0)
            halves.append(dot(wyi[p], lines))
        for s, out in enumerate((halves[0] + halves[1], halves[0] - halves[1])):
            for c in range(2):
                for to in range(ny // 2):
                    at = base + (s * (ny // 2) + to) * xrow + 2 * i * yl + c
                    bbuf[pl.ds(at, yl, stride=2), :] = out[c * half + to * yl:c * half + (to + 1) * yl]

    x_prefetch(0)
    tables[0].start()
    for o in range(1, ny):
        pl.semaphore_signal(barrier, inc=1, device_id={"py": lax.rem(py + o, ny)}, device_id_type=MESH)
    for o in range(1, nz):
        pl.semaphore_signal(barrier, inc=1, device_id={"pz": lax.rem(pz + o, nz)}, device_id_type=MESH)
    tables[0].wait()
    x_forward(0, 0, groups)
    for c in range(2):
        g_copy(c, 0).start()
        g_copy(c, 1).start()
    for table in tables[1:]:
        table.start()
    x_prefetch(0)
    for jj in range(1, HALF_X_CHUNKS):
        for o in x_offsets:
            xf(jj, o).start()
    for table in tables[1:]:
        table.wait()

    def step(t, carry):
        @pl.when(t < nj)
        def _():
            xf_wait(t)
            y_forward(t)
            for o in y_offsets:
                yf(t, o).start()

        @pl.when((t >= 1) & (t < nj + 1))
        def _():
            j = t - 1
            yf_wait(j)
            for c in range(2):
                g_copy(c, j).wait()
            z_solve(j)
            for i in range(kc):
                for o in y_offsets:
                    for c in range(2):
                        yi(j, o, (c * kc + i) * zl, zl, i).start()

            @pl.when(j + 2 < nj)
            def _():
                for c in range(2):
                    g_copy(c, j + 2).start()

        @pl.when(t >= 2)
        def _():
            j = t - 2
            own(cbuf, dbuf, j, pz, yrow)
            for i in range(kc):
                yi_wait(j, i)
                y_inverse(j, i)
                for o in x_offsets:
                    xi(j, o, 2 * i * yl, 2 * yl, i).start()
            own(bbuf, ebuf, j, py, xrow)

        @pl.when(t < 4)
        def _():
            x_forward(1, t * piece, (t + 1) * piece)

            @pl.when(t < 3)
            def _():
                x_prefetch((t + 1) * piece)

        @pl.when(t == 3)
        def _():
            def send(jj, c):
                for o in x_offsets:
                    xf(jj, o).start()
                return c

            lax.fori_loop(HALF_X_CHUNKS, nj, send, 0)

        @pl.when(t == nj - 4)
        def _():
            for jj in range(HALF_X_CHUNKS):
                for i in range(kc):
                    xi_wait(jj, i)

        @pl.when((t >= nj - 4) & (t < nj))
        def _():
            def body(k, c):
                group = (t - (nj - 4)) * piece + k
                even[group] = x_inverse(ebuf, wx, 0, group, ny, crow, xrow)
                return c

            lax.fori_loop(0, piece, body, 0)

        return carry

    lax.fori_loop(0, nj + 2, step, 0)
    for jj in range(HALF_X_CHUNKS, nj):
        for i in range(kc):
            xi_wait(jj, i)


def x_inverse(ebuf, wx, p, group, ny, crow, xrow):
    def tile(jj, src, i):
        at = (p * HALF_X_CHUNKS + jj) * crow + src * xrow + i * (xrow // 2) + group * 8
        return ebuf[pl.ds(pl.multiple_of(at, 8), 8), :]

    quads = [jnp.concatenate([tile(jj, src + k // 2, k % 2) for jj in range(HALF_X_CHUNKS) for src in range(0, ny, 2)], axis=0)
             for k in range(4)]
    a0, a2 = swap_rows(quads[0], quads[2])
    a1, a3 = swap_rows(quads[1], quads[3])
    lines = [v.reshape(-1, LANES) for v in (*swap_pairs(a0, a1), *swap_pairs(a2, a3))]
    return dot(jnp.concatenate(lines, axis=1), wx[p], ((0,), (0,)))


def finish(ny, n, nf, ebuf, even, hat_re, hat_im, wx, phi_re, phi_im, out_re, out_im, stage, p_sem, h_sem):
    half = n // 2
    yl = n // ny
    nj = 2 * HALF_X_CHUNKS
    crow = ebuf.shape[0] // nj
    xrow = crow // ny
    zl = phi_re.shape[2]
    phi = (phi_re, phi_im)
    hats = [pltpu.make_async_copy(a, b, h_sem.at[c]) for c, (a, b) in enumerate(((hat_re, out_re), (hat_im, out_im)))]
    for h in hats:
        h.start()

    def phi_copy(c, group):
        slot = lax.rem(group, OUT_SLOTS)
        return pltpu.make_async_copy(stage.at[slot, c], phi[c].at[:, pl.ds(4 * group, 4)], p_sem.at[slot, c])

    def body(group, carry):
        @pl.when(group >= OUT_SLOTS)
        def _():
            for c in range(2):
                phi_copy(c, group - OUT_SLOTS).wait()

        slot = lax.rem(group, OUT_SLOTS)
        e, o = even[group], x_inverse(ebuf, wx, 1, group, ny, crow, xrow)
        for c in range(2):
            ec, oc = e[:, c * half:(c + 1) * half], o[:, c * half:(c + 1) * half]
            out = jnp.concatenate([ec + oc, ec - oc], axis=1).reshape(4, nf, zl, n)
            stage[slot, c] = jnp.swapaxes(out, 0, 1)
        for c in range(2):
            phi_copy(c, group).start()
        return carry

    groups = yl // 4
    lax.fori_loop(0, groups, body, 0)
    for group in range(groups - OUT_SLOTS, groups):
        for c in range(2):
            phi_copy(c, group).wait()
    for h in hats:
        h.wait()


def solution(mesh):
    ny, nz = mesh.shape["py"], mesh.shape["pz"]

    def local_solve(rho_re, rho_im, g_re, g_im):
        nf, n, yl, zl = rho_re.shape
        kl, ml = g_re.shape[:2]
        kc = kl // HALF_X_CHUNKS // 2
        nj = 2 * HALF_X_CHUNKS
        rows = nj * ny * yl * 2 * kc
        tables = [jnp.asarray(w) for w in dft_tables(n, ny, nz)]
        space = jax.ShapeDtypeStruct((nf, yl, zl, n), jnp.float32)
        wave_shape = (nf, kl // 2, 2, ml, n)
        wave = jax.ShapeDtypeStruct(wave_shape, jnp.float32)
        dma = pltpu.SemaphoreType.DMA
        buf = pltpu.VMEM((rows, LANES), jnp.float32)
        vmem = pl.BlockSpec(memory_space=pltpu.VMEM)
        hbm = pl.BlockSpec(memory_space=pl.ANY)
        inner = pl.pallas_call(
            functools.partial(kernel, ny, nz, n, nf),
            out_shape=(pltpu.VMEM((rows, LANES), jnp.float32), pltpu.VMEM((yl // 4, 4 * nf * zl, n), jnp.float32),
                       pltpu.VMEM(wave_shape, jnp.float32), pltpu.VMEM(wave_shape, jnp.float32)),
            in_specs=[hbm] * 8,
            out_specs=[vmem] * 4,
            scratch_shapes=[
                buf, buf, buf, buf,
                pltpu.VMEM((SLOTS, 2, nf, 2 * GROUP, zl, n), jnp.float32),
                pltpu.VMEM((2, 2, kc, ml, n), jnp.float32),
                *[pltpu.VMEM(t.shape, jnp.float32) for t in tables],
                *[dma((nj,)) for _ in range(4)], *[dma((nj, kc)) for _ in range(4)],
                dma((len(tables),)), dma((SLOTS, 2)), dma((2, 2)),
            ],
            compiler_params=pltpu.CompilerParams(
                collective_id=0, has_side_effects=True, vmem_limit_bytes=INNER_VMEM),
            name="spectral",
        )(jnp.transpose(rho_re, (0, 2, 3, 1)), jnp.transpose(rho_im, (0, 2, 3, 1)),
          g_re.reshape(kl // 2, 2, ml, n), g_im.reshape(kl // 2, 2, ml, n), *tables)
        outs = pl.pallas_call(
            functools.partial(finish, ny, n, nf),
            out_shape=(space, space, wave, wave),
            in_specs=[vmem] * 5,
            out_specs=[hbm] * 4,
            scratch_shapes=[pltpu.VMEM((OUT_SLOTS, 2, nf, 4, zl, n), jnp.float32), dma((OUT_SLOTS, 2)), dma((2,))],
            compiler_params=pltpu.CompilerParams(vmem_limit_bytes=16 << 20),
            name="finish",
        )(*inner, tables[0])
        phi = [jnp.transpose(v, (0, 3, 1, 2)) for v in outs[:2]]
        return (*phi, *(v.reshape(nf, kl, ml, n) for v in outs[2:]))

    space_layout = P("dp", None, "py", "pz")
    wave_layout = P("dp", "py", "pz", None)
    green_layout = P("py", "pz", None)
    return jax.shard_map(local_solve, mesh=mesh,
                         in_specs=(space_layout, space_layout, green_layout, green_layout),
                         out_specs=(space_layout, space_layout, wave_layout, wave_layout),
                         check_vma=False)
```

```python
import functools

import jax
import jax.numpy as jnp
import numpy as np
from jax import lax
from jax.experimental import pallas as pl
from jax.experimental.pallas import tpu as pltpu
from jax.sharding import PartitionSpec as P

MESH = pl.DeviceIdType.MESH
HALF_X_CHUNKS = 8
SLOTS = 3
GROUP = 2
OUT_SLOTS = 4
DEPTH = 4
LANES = 128
INNER_VMEM = 42 << 20


def real_form(matrix):
    return np.block([[matrix.real, -matrix.imag], [matrix.imag, matrix.real]])


def dft_tables(n, ny, nz):
    half = n // 2
    scale = 1.0 / np.sqrt(n)
    low, full = np.arange(half), np.arange(n)
    dft = lambda k, j, sign: scale * np.exp(sign * 2j * np.pi * ((k[:, None] * j[None, :]) % n) / n)
    per = n // ny // HALF_X_CHUNKS // 2
    order = np.arange(half).reshape(ny, HALF_X_CHUNKS, per).transpose(1, 0, 2)
    rows = np.stack([order, order + half], axis=3).reshape(-1)
    wx = np.stack([real_form(dft(2 * low + p, low, -1))[rows] for p in range(2)])
    wy = np.stack([real_form(dft(2 * low + p, low, -1)) for p in range(2)])
    wyi = np.stack([real_form(dft(low, 2 * low + p, 1)) for p in range(2)])
    lz = n // nz
    zrows = np.arange(n).reshape(nz, lz)
    zrows = np.stack([zrows, zrows + n], axis=1).reshape(-1)
    wz = real_form(dft(full, full, -1)).T[zrows]
    return [np.asarray(w, np.float32) for w in (wx, wy, wz, wyi)]


def dot(a, b, dims=((1,), (0,))):
    return lax.dot_general(a, b, (dims, ((), ())), precision=lax.Precision.HIGHEST,
                           preferred_element_type=jnp.float32)


def swap_rows(first, second):
    a, b = first.reshape(-1, 8, LANES), second.reshape(-1, 8, LANES)
    upper = lax.broadcasted_iota(jnp.int32, a.shape, 1) < 4
    return jnp.where(upper, a, pltpu.roll(b, 4, 1)), jnp.where(upper, pltpu.roll(a, 4, 1), b)


def swap_pairs(a, b):
    kept = lax.broadcasted_iota(jnp.int32, a.shape, 1) & 2 == 0
    return jnp.where(kept, a, pltpu.roll(b, 2, 1)), jnp.where(kept, pltpu.roll(a, 6, 1), b)


def kernel(ny, nz, n, nf,
           rho_re, rho_im, g_re, g_im, wx_h, wy_h, wz_h, wyi_h,
           ebuf, even, hat_re, hat_im,
           abuf, bbuf, cbuf, dbuf, stage, gbuf, wx, wy, wz, wyi,
           xs, xr, ys, yr, yis, yir, xis, xir, w_sem, in_sem, g_sem):
    py, pz = lax.axis_index("py"), lax.axis_index("pz")
    half = n // 2
    yl, zl = n // ny, n // nz
    kc = n // ny // HALF_X_CHUNKS // 2
    nj = 2 * HALF_X_CHUNKS
    xrow, yrow = yl * 2 * kc, 2 * kc * zl
    crow = ny * xrow
    pairs = yl // 2
    groups = pairs // GROUP
    piece = groups // 4
    early, late, odd = range(HALF_X_CHUNKS // 2), range(HALF_X_CHUNKS // 2, HALF_X_CHUNKS), range(HALF_X_CHUNKS)
    sends = [(k, 2) for k in range(0, groups - 2, 2)] + [(groups - 2, 1), (groups - 1, 1)]
    rho, gg, hat = (rho_re, rho_im), (g_re, g_im), (hat_re, hat_im)
    x_offsets = (4, 3, 5, 2, 6, 1, 7) if ny == 8 else tuple(range(1, ny))
    y_offsets = (2, 1, 3) if nz == 4 else tuple(range(1, nz))

    barrier = pltpu.get_barrier_semaphore()
    tables = [pltpu.make_async_copy(h, v, w_sem.at[i]) for i, (h, v) in enumerate(
        ((wx_h, wx), (wy_h, wy), (wz_h, wz), (wyi_h, wyi)))]

    def rho_copy(c, group):
        slot = lax.rem(group, SLOTS)
        return pltpu.make_async_copy(rho[c].at[:, pl.ds(2 * GROUP * group, 2 * GROUP)], stage.at[slot, c],
                                     in_sem.at[slot, c])

    def g_copy(c, j):
        p, jj, slot = j // HALF_X_CHUNKS, lax.rem(j, HALF_X_CHUNKS), lax.rem(j, 2)
        return pltpu.make_async_copy(gg[c].at[pl.ds(kc * jj, kc), p], gbuf.at[slot, c], g_sem.at[slot, c])

    def x_copy(src, dst, ss, rs, j, o, first=0, count=None, sem=None):
        to = lax.rem(py + o, ny)
        rows = xrow if count is None else count
        return pltpu.make_async_remote_copy(
            src.at[pl.ds(pl.multiple_of(j * crow + to * xrow + first, 8), rows)],
            dst.at[pl.ds(pl.multiple_of(j * crow + py * xrow + first, 8), rows)],
            ss.at[j if sem is None else sem], rs.at[j if sem is None else sem],
            device_id={"py": to}, device_id_type=MESH)

    def y_copy(src, dst, ss, rs, j, o, first=0, count=None, *half_of):
        sem = (lax.rem(j, ys.shape[0]), *half_of)
        to = lax.rem(pz + o, nz)
        rows = yrow if count is None else count
        return pltpu.make_async_remote_copy(
            src.at[pl.ds(pl.multiple_of(j * crow + to * yrow + first, 8), rows)],
            dst.at[pl.ds(pl.multiple_of(j * crow + pz * yrow + first, 8), rows)],
            ss.at[*sem], rs.at[*sem], device_id={"pz": to}, device_id_type=MESH)

    def await_all(src, dst, ss, rs, axis, me, size, rows, *of):
        at = pl.ds(pl.multiple_of(of[0] * crow, 8), rows)
        pltpu.make_async_remote_copy(src.at[at], dst.at[at], ss.at[lax.rem(of[0], ss.shape[0]), *of[1:]], rs.at[lax.rem(of[0], ss.shape[0]), *of[1:]],
                                     device_id={axis: lax.rem(me + 1, size)}, device_id_type=MESH).wait()

    def own(src, dst, j, mine, rows):
        at = pl.ds(pl.multiple_of(j * crow + mine * rows, 8), rows)
        dst[at, :] = src[at, :]

    xf = functools.partial(x_copy, abuf, bbuf, xs, xr)
    yf = functools.partial(y_copy, abuf, cbuf, ys, yr)
    yi = functools.partial(y_copy, cbuf, dbuf, yis, yir)
    xi = functools.partial(x_copy, bbuf, ebuf, xis, xir)
    xf_wait = functools.partial(await_all, abuf, bbuf, xs, xr, "py", py, ny, (ny - 1) * xrow)
    yf_wait = functools.partial(await_all, abuf, cbuf, ys, yr, "pz", pz, nz, (nz - 1) * yrow)
    yi_wait = functools.partial(await_all, cbuf, dbuf, yis, yir, "pz", pz, nz, (nz - 1) * yrow // 2)
    def xi_wait(p):
        at = pl.ds(p * HALF_X_CHUNKS * crow, HALF_X_CHUNKS * (ny - 1) * xrow)
        pltpu.make_async_remote_copy(bbuf.at[at], ebuf.at[at], xis.at[p], xir.at[p],
                                     device_id={"py": lax.rem(py + 1, ny)}, device_id_type=MESH).wait()

    def x_prefetch(first):
        for k in range(SLOTS - 1):
            for c in range(2):
                rho_copy(c, first + k).start()

    def x_forward(p, jjs, first, stop):
        def body(group, carry):
            @pl.when(group + SLOTS - 1 < stop)
            def _():
                for c in range(2):
                    rho_copy(c, group + SLOTS - 1).start()

            for c in range(2):
                rho_copy(c, group).wait()
            slot = lax.rem(group, SLOTS)
            folded = []
            for c in range(2):
                lines = stage[slot, c]
                low, high = lines[..., :half], lines[..., half:]
                both = low - high if p else low + high
                folded.append(jnp.swapaxes(both, 0, 1).reshape(2 * GROUP * nf * zl, half))
            per_jj = ny * 2 * kc
            out = dot(wx[p, jjs[0] * per_jj:(jjs[-1] + 1) * per_jj], jnp.concatenate(folded, axis=1), ((1,), (1,)))
            for u in range(GROUP):
                blocks = swap_rows(out[:, 2 * u * LANES:(2 * u + 1) * LANES],
                                   out[:, (2 * u + 1) * LANES:(2 * u + 2) * LANES])
                for jj in jjs:
                    for to in range(ny):
                        r = (jj - jjs[0]) * ny + to
                        at = (p * HALF_X_CHUNKS + jj) * crow + to * xrow + (group * GROUP + u) * 8
                        abuf[pl.ds(pl.multiple_of(at, 8), 8), :] = blocks[r % 2][r // 2]
            if p == 0 and jjs[0] == 0:
                for start, count in sends:
                    @pl.when(group == start + count - 1)
                    def _():
                        if start == 0:
                            pl.semaphore_wait(barrier, ny + nz - 2)
                        for o in x_offsets:
                            xf(0, o, start * GROUP * 8, count * GROUP * 8).start()
            return carry

        lax.fori_loop(first, stop, body, 0)

    def y_forward(j):
        own(abuf, bbuf, j, py, xrow)
        base = j * crow
        parts = []
        for c in range(2):
            parts.append(jnp.concatenate(
                [bbuf[pl.ds(base + 2 * i + c, n, stride=2 * kc), :] for i in range(2)], axis=1))
        for p in range(2):
            folded = jnp.concatenate([v[:half] - v[half:] if p else v[:half] + v[half:] for v in parts], axis=0)
            out = dot(wy[p], folded)
            for c in range(2):
                for to in range(nz):
                    for k in range(2):
                        at = base + to * yrow + (c * kc + k) * zl + p
                        abuf[pl.ds(at, zl // 2, stride=2), :] = out[
                            c * half + to * zl // 2:c * half + (to + 1) * zl // 2, k * LANES:(k + 1) * LANES]

    def z_solve(j):
        own(abuf, cbuf, j, pz, yrow)
        base, slot = j * crow, lax.rem(j, 2)
        p, jj = j // HALF_X_CHUNKS, lax.rem(j, HALF_X_CHUNKS)
        rows = kc * zl
        left = lax.broadcasted_iota(jnp.int32, (rows, LANES), 1) < zl
        swap = lambda v: pltpu.roll(v, zl, 1)
        lines = ([], [])
        for b in range(nz):
            at = base + b * yrow
            re = cbuf[pl.ds(pl.multiple_of(at, 8), rows), :]
            im = cbuf[pl.ds(pl.multiple_of(at + rows, 8), rows), :]
            lines[0].append(jnp.where(left, re, swap(im)))
            lines[1].append(jnp.where(left, swap(re), im))
        both = jnp.concatenate([jnp.concatenate(v, axis=1) for v in lines], axis=0)
        spec = dot(both, wz[...])
        gr = gbuf[slot, 0].reshape(rows, n)
        gi = gbuf[slot, 1].reshape(rows, n)
        scaled = []
        for f in range(nf):
            sr, si = spec[f * rows:(f + 1) * rows, :n], spec[f * rows:(f + 1) * rows, n:]
            hr, hi = sr * gr - si * gi, sr * gi + si * gr
            hat_re[f, pl.ds(kc * jj, kc), p] = hr.reshape(kc, zl, n)
            hat_im[f, pl.ds(kc * jj, kc), p] = hi.reshape(kc, zl, n)
            scaled.append(jnp.concatenate([hr, hi], axis=1))
        back = dot(jnp.concatenate(scaled, axis=0), wz[...], ((1,), (1,)))
        for b in range(nz):
            first, second = (back[f * rows:(f + 1) * rows, b * LANES:(b + 1) * LANES] for f in range(2))
            at = base + b * yrow
            cbuf[pl.ds(pl.multiple_of(at, 8), rows), :] = jnp.where(left, first, swap(second))
            cbuf[pl.ds(pl.multiple_of(at + rows, 8), rows), :] = jnp.where(left, swap(first), second)

    def y_inverse(j, i):
        base = j * crow
        halves = []
        for p in range(2):
            lines = jnp.concatenate(
                [dbuf[pl.ds(base + src * yrow + (c * kc + i) * zl + p, zl // 2, stride=2), :]
                 for c in range(2) for src in range(nz)], axis=0)
            halves.append(dot(wyi[p], lines))
        for s, out in enumerate((halves[0] + halves[1], halves[0] - halves[1])):
            for c in range(2):
                for to in range(ny // 2):
                    at = base + (s * (ny // 2) + to) * xrow + 2 * i * yl + c
                    bbuf[pl.ds(at, yl, stride=2), :] = out[c * half + to * yl:c * half + (to + 1) * yl]

    x_prefetch(0)
    tables[0].start()
    for o in range(1, ny):
        pl.semaphore_signal(barrier, inc=1, device_id={"py": lax.rem(py + o, ny)}, device_id_type=MESH)
    for o in range(1, nz):
        pl.semaphore_signal(barrier, inc=1, device_id={"pz": lax.rem(pz + o, nz)}, device_id_type=MESH)
    tables[0].wait()
    x_forward(0, early, 0, groups)
    for c in range(2):
        g_copy(c, 0).start()
        g_copy(c, 1).start()
    for table in tables[1:]:
        table.start()
    x_prefetch(0)
    for jj in early[1:]:
        for o in x_offsets:
            xf(jj, o).start()
    for table in tables[1:]:
        table.wait()

    def step(t, carry):
        @pl.when(t < nj)
        def _():
            xf_wait(t)
            y_forward(t)
            for o in y_offsets:
                yf(t, o).start()

        @pl.when((t >= 1) & (t < nj + 1))
        def _():
            j = t - 1
            yf_wait(j)
            for c in range(2):
                g_copy(c, j).wait()
            z_solve(j)
            for i in range(kc):
                for o in y_offsets:
                    for c in range(2):
                        yi(j, o, (c * kc + i) * zl, zl, i).start()

            @pl.when(j + 2 < nj)
            def _():
                for c in range(2):
                    g_copy(c, j + 2).start()

        @pl.when(t >= 2)
        def _():
            j = t - 2
            own(cbuf, dbuf, j, pz, yrow)
            for i in range(kc):
                yi_wait(j, i)
                y_inverse(j, i)
                for o in x_offsets:
                    xi(j, o, 2 * i * yl, 2 * yl, j // HALF_X_CHUNKS).start()
            own(bbuf, ebuf, j, py, xrow)

        def spare(p, jjs, begin):
            part = groups // 2

            def send(j, c):
                for o in x_offsets:
                    xf(j, o).start()
                return c

            @pl.when((t >= begin) & (t < begin + 2))
            def _():
                x_forward(p, jjs, (t - begin) * part, (t - begin + 1) * part)
                if p == 0:
                    x_prefetch(jnp.where(t == begin, part, 0))
                else:
                    @pl.when(t == begin)
                    def _():
                        x_prefetch(part)

            @pl.when(t == begin + 1)
            def _():
                base = p * HALF_X_CHUNKS
                lax.fori_loop(base + jjs[0], base + jjs[-1] + 1, send, 0)

        spare(0, late, 0)
        spare(1, odd, 2)

        @pl.when(t == nj - 4)
        def _():
            xi_wait(0)

        @pl.when((t >= nj - 4) & (t < nj))
        def _():
            def body(k, c):
                group = (t - (nj - 4)) * piece + k
                even[group] = x_inverse(ebuf, wx, 0, group, ny, crow, xrow)
                return c

            lax.fori_loop(0, piece, body, 0)

        return carry

    lax.fori_loop(0, nj + 2, step, 0)
    xi_wait(1)


def x_inverse(ebuf, wx, p, group, ny, crow, xrow):
    def tile(jj, src, i):
        at = (p * HALF_X_CHUNKS + jj) * crow + src * xrow + i * (xrow // 2) + group * 8
        return ebuf[pl.ds(pl.multiple_of(at, 8), 8), :]

    quads = [jnp.concatenate([tile(jj, src + k // 2, k % 2) for jj in range(HALF_X_CHUNKS) for src in range(0, ny, 2)], axis=0)
             for k in range(4)]
    a0, a2 = swap_rows(quads[0], quads[2])
    a1, a3 = swap_rows(quads[1], quads[3])
    lines = [v.reshape(-1, LANES) for v in (*swap_pairs(a0, a1), *swap_pairs(a2, a3))]
    return dot(jnp.concatenate(lines, axis=1), wx[p], ((0,), (0,)))


def finish(ny, n, nf, ebuf, even, hat_re, hat_im, wx, phi_re, phi_im, out_re, out_im, stage, p_sem, h_sem):
    half = n // 2
    yl = n // ny
    nj = 2 * HALF_X_CHUNKS
    crow = ebuf.shape[0] // nj
    xrow = crow // ny
    zl = phi_re.shape[2]
    phi = (phi_re, phi_im)
    hats = [pltpu.make_async_copy(a, b, h_sem.at[c]) for c, (a, b) in enumerate(((hat_re, out_re), (hat_im, out_im)))]
    for h in hats:
        h.start()

    def phi_copy(c, group):
        slot = lax.rem(group, OUT_SLOTS)
        return pltpu.make_async_copy(stage.at[slot, c], phi[c].at[:, pl.ds(4 * group, 4)], p_sem.at[slot, c])

    def body(group, carry):
        @pl.when(group >= OUT_SLOTS)
        def _():
            for c in range(2):
                phi_copy(c, group - OUT_SLOTS).wait()

        slot = lax.rem(group, OUT_SLOTS)
        e, o = even[group], x_inverse(ebuf, wx, 1, group, ny, crow, xrow)
        for c in range(2):
            ec, oc = e[:, c * half:(c + 1) * half], o[:, c * half:(c + 1) * half]
            out = jnp.concatenate([ec + oc, ec - oc], axis=1).reshape(4, nf, zl, n)
            stage[slot, c] = jnp.swapaxes(out, 0, 1)
        for c in range(2):
            phi_copy(c, group).start()
        return carry

    groups = yl // 4
    lax.fori_loop(0, groups, body, 0)
    for group in range(groups - OUT_SLOTS, groups):
        for c in range(2):
            phi_copy(c, group).wait()
    for h in hats:
        h.wait()


def solution(mesh):
    ny, nz = mesh.shape["py"], mesh.shape["pz"]

    def local_solve(rho_re, rho_im, g_re, g_im):
        nf, n, yl, zl = rho_re.shape
        kl, ml = g_re.shape[:2]
        kc = kl // HALF_X_CHUNKS // 2
        nj = 2 * HALF_X_CHUNKS
        rows = nj * ny * yl * 2 * kc
        tables = [jnp.asarray(w) for w in dft_tables(n, ny, nz)]
        space = jax.ShapeDtypeStruct((nf, yl, zl, n), jnp.float32)
        wave_shape = (nf, kl // 2, 2, ml, n)
        wave = jax.ShapeDtypeStruct(wave_shape, jnp.float32)
        dma = pltpu.SemaphoreType.DMA
        buf = pltpu.VMEM((rows, LANES), jnp.float32)
        vmem = pl.BlockSpec(memory_space=pltpu.VMEM)
        hbm = pl.BlockSpec(memory_space=pl.ANY)
        inner = pl.pallas_call(
            functools.partial(kernel, ny, nz, n, nf),
            out_shape=(pltpu.VMEM((rows, LANES), jnp.float32), pltpu.VMEM((yl // 4, 4 * nf * zl, n), jnp.float32),
                       pltpu.VMEM(wave_shape, jnp.float32), pltpu.VMEM(wave_shape, jnp.float32)),
            in_specs=[hbm] * 8,
            out_specs=[vmem] * 4,
            scratch_shapes=[
                buf, buf, buf, buf,
                pltpu.VMEM((SLOTS, 2, nf, 2 * GROUP, zl, n), jnp.float32),
                pltpu.VMEM((2, 2, kc, ml, n), jnp.float32),
                *[pltpu.VMEM(t.shape, jnp.float32) for t in tables],
                dma((nj,)), dma((nj,)), dma((DEPTH,)), dma((DEPTH,)),
                dma((DEPTH, kc)), dma((DEPTH, kc)), dma((2,)), dma((2,)),
                dma((len(tables),)), dma((SLOTS, 2)), dma((2, 2)),
            ],
            compiler_params=pltpu.CompilerParams(
                collective_id=0, has_side_effects=True, vmem_limit_bytes=INNER_VMEM),
            name="spectral",
        )(jnp.transpose(rho_re, (0, 2, 3, 1)), jnp.transpose(rho_im, (0, 2, 3, 1)),
          g_re.reshape(kl // 2, 2, ml, n), g_im.reshape(kl // 2, 2, ml, n), *tables)
        outs = pl.pallas_call(
            functools.partial(finish, ny, n, nf),
            out_shape=(space, space, wave, wave),
            in_specs=[vmem] * 5,
            out_specs=[hbm] * 4,
            scratch_shapes=[pltpu.VMEM((OUT_SLOTS, 2, nf, 4, zl, n), jnp.float32), dma((OUT_SLOTS, 2)), dma((2,))],
            compiler_params=pltpu.CompilerParams(vmem_limit_bytes=16 << 20),
            name="finish",
        )(*inner, tables[0])
        phi = [jnp.transpose(v, (0, 3, 1, 2)) for v in outs[:2]]
        return (*phi, *(v.reshape(nf, kl, ml, n) for v in outs[2:]))

    space_layout = P("dp", None, "py", "pz")
    wave_layout = P("dp", "py", "pz", None)
    green_layout = P("py", "pz", None)
    return jax.shard_map(local_solve, mesh=mesh,
                         in_specs=(space_layout, space_layout, green_layout, green_layout),
                         out_specs=(space_layout, space_layout, wave_layout, wave_layout),
                         check_vma=False)
```

```python
import functools

import jax
import jax.numpy as jnp
import numpy as np
from jax import lax
from jax.experimental import pallas as pl
from jax.experimental.pallas import tpu as pltpu
from jax.sharding import PartitionSpec as P

MESH = pl.DeviceIdType.MESH
HALF_X_CHUNKS = 8
SLOTS = 3
GROUP = 2
OUT_SLOTS = 6
REFINE_EARLY = 3
DEPTH = 4
SPLIT = 4
LANES = 128
INNER_VMEM = 35 << 20


def real_form(matrix):
    return np.block([[matrix.real, -matrix.imag], [matrix.imag, matrix.real]])


def dft_tables(n, ny, nz):
    half = n // 2
    scale = 1.0 / np.sqrt(n)
    low, full = np.arange(half), np.arange(n)
    dft = lambda k, j, sign: scale * np.exp(sign * 2j * np.pi * ((k[:, None] * j[None, :]) % n) / n)
    per = n // ny // HALF_X_CHUNKS // 2
    order = np.arange(half).reshape(ny, HALF_X_CHUNKS, per).transpose(1, 0, 2)
    rows = np.stack([order, order + half], axis=3).reshape(-1)
    wx = np.stack([real_form(dft(2 * low + p, low, -1))[rows] for p in range(2)])
    wy = np.stack([real_form(dft(2 * low + p, low, -1)) for p in range(2)])
    wyi = np.stack([real_form(dft(low, 2 * low + p, 1)) for p in range(2)])
    lz = n // nz
    zrows = np.arange(n).reshape(nz, lz)
    zrows = np.stack([zrows, zrows + n], axis=1).reshape(-1)
    wz = real_form(dft(full, full, -1)).T[zrows]
    return [np.asarray(w, np.float32) for w in (wx, wy, wz, wyi)]


def dot(a, b, dims=((1,), (0,))):
    return lax.dot_general(a, b, (dims, ((), ())), precision=lax.Precision.HIGHEST,
                           preferred_element_type=jnp.float32)


def swap_rows(first, second):
    a, b = first.reshape(-1, 8, LANES), second.reshape(-1, 8, LANES)
    upper = lax.broadcasted_iota(jnp.int32, a.shape, 1) < 4
    return jnp.where(upper, a, pltpu.roll(b, 4, 1)), jnp.where(upper, pltpu.roll(a, 4, 1), b)


def swap_pairs(a, b):
    kept = lax.broadcasted_iota(jnp.int32, a.shape, 1) & 2 == 0
    return jnp.where(kept, a, pltpu.roll(b, 2, 1)), jnp.where(kept, pltpu.roll(a, 6, 1), b)


def kernel(ny, nz, n, nf,
           rho_re, rho_im, g_re, g_im, wx_h, wy_h, wz_h, wyi_h,
           ebuf, abuf, hat_re, hat_im,
           bbuf, cbuf, dbuf, stage, gbuf, wx, wy, wz, wyi,
           xs, xr, ys, yr, yis, yir, xis, xir, w_sem, in_sem, g_sem):
    py, pz = lax.axis_index("py"), lax.axis_index("pz")
    half = n // 2
    yl, zl = n // ny, n // nz
    kc = n // ny // HALF_X_CHUNKS // 2
    nj = 2 * HALF_X_CHUNKS
    xrow, yrow = yl * 2 * kc, 2 * kc * zl
    crow = ny * xrow
    pairs = yl // 2
    groups = pairs // GROUP
    piece = groups // 4
    early, late, odd = range(HALF_X_CHUNKS // 2), range(HALF_X_CHUNKS // 2, HALF_X_CHUNKS), range(HALF_X_CHUNKS)
    sends = [(k, 2) for k in range(0, groups - 2, 2)] + [(groups - 2, 1), (groups - 1, 1)]
    rho, gg, hat = (rho_re, rho_im), (g_re, g_im), (hat_re, hat_im)
    x_offsets = (4, 3, 5, 2, 6, 1, 7) if ny == 8 else tuple(range(1, ny))
    y_offsets = (2, 1, 3) if nz == 4 else tuple(range(1, nz))

    barrier = pltpu.get_barrier_semaphore()
    tables = [pltpu.make_async_copy(h, v, w_sem.at[i]) for i, (h, v) in enumerate(
        ((wx_h, wx), (wy_h, wy), (wz_h, wz), (wyi_h, wyi)))]

    def rho_copy(c, group):
        slot = lax.rem(group, SLOTS)
        return pltpu.make_async_copy(rho[c].at[:, pl.ds(2 * GROUP * group, 2 * GROUP)], stage.at[slot, c],
                                     in_sem.at[slot, c])

    def g_copy(c, j):
        p, jj, slot = j // HALF_X_CHUNKS, lax.rem(j, HALF_X_CHUNKS), lax.rem(j, 2)
        return pltpu.make_async_copy(gg[c].at[pl.ds(kc * jj, kc), p], gbuf.at[slot, c], g_sem.at[slot, c])

    def x_copy(src, dst, ss, rs, j, o, first=0, count=None, sem=None):
        to = lax.rem(py + o, ny)
        rows = xrow if count is None else count
        return pltpu.make_async_remote_copy(
            src.at[pl.ds(pl.multiple_of(j * crow + to * xrow + first, 8), rows)],
            dst.at[pl.ds(pl.multiple_of(j * crow + py * xrow + first, 8), rows)],
            ss.at[j if sem is None else sem], rs.at[j if sem is None else sem],
            device_id={"py": to}, device_id_type=MESH)

    def y_copy(src, dst, ss, rs, j, o, first=0, count=None, *half_of):
        sem = (lax.rem(j, ys.shape[0]), *half_of)
        to = lax.rem(pz + o, nz)
        rows = yrow if count is None else count
        return pltpu.make_async_remote_copy(
            src.at[pl.ds(pl.multiple_of(j * crow + to * yrow + first, 8), rows)],
            dst.at[pl.ds(pl.multiple_of(j * crow + pz * yrow + first, 8), rows)],
            ss.at[*sem], rs.at[*sem], device_id={"pz": to}, device_id_type=MESH)

    def await_all(src, dst, ss, rs, axis, me, size, rows, *of):
        at = pl.ds(pl.multiple_of(of[0] * crow, 8), rows)
        pltpu.make_async_remote_copy(src.at[at], dst.at[at], ss.at[lax.rem(of[0], ss.shape[0]), *of[1:]], rs.at[lax.rem(of[0], ss.shape[0]), *of[1:]],
                                     device_id={axis: lax.rem(me + 1, size)}, device_id_type=MESH).wait()

    def own(src, dst, j, mine, rows):
        at = pl.ds(pl.multiple_of(j * crow + mine * rows, 8), rows)
        dst[at, :] = src[at, :]

    xf = functools.partial(x_copy, abuf, bbuf, xs, xr)
    yf = functools.partial(y_copy, abuf, cbuf, ys, yr)
    yi = functools.partial(y_copy, cbuf, dbuf, yis, yir)
    xi = functools.partial(x_copy, bbuf, ebuf, xis, xir)
    xf_wait = functools.partial(await_all, abuf, bbuf, xs, xr, "py", py, ny, (ny - 1) * xrow)
    yf_wait = functools.partial(await_all, abuf, cbuf, ys, yr, "pz", pz, nz, (nz - 1) * yrow)
    yi_wait = functools.partial(await_all, cbuf, dbuf, yis, yir, "pz", pz, nz, (nz - 1) * yrow // 2)
    cuts = (0, HALF_X_CHUNKS, HALF_X_CHUNKS + SPLIT, nj)

    def xi_wait(k):
        at = pl.ds(cuts[k] * crow, (cuts[k + 1] - cuts[k]) * (ny - 1) * xrow)
        pltpu.make_async_remote_copy(bbuf.at[at], ebuf.at[at], xis.at[k], xir.at[k],
                                     device_id={"py": lax.rem(py + 1, ny)}, device_id_type=MESH).wait()

    def x_prefetch(first):
        for k in range(SLOTS - 1):
            for c in range(2):
                rho_copy(c, first + k).start()

    def x_forward(p, jjs, first, stop):
        def body(group, carry):
            @pl.when(group + SLOTS - 1 < stop)
            def _():
                for c in range(2):
                    rho_copy(c, group + SLOTS - 1).start()

            for c in range(2):
                rho_copy(c, group).wait()
            slot = lax.rem(group, SLOTS)
            folded = []
            for c in range(2):
                lines = stage[slot, c]
                low, high = lines[..., :half], lines[..., half:]
                both = low - high if p else low + high
                folded.append(jnp.swapaxes(both, 0, 1).reshape(2 * GROUP * nf * zl, half))
            per_jj = ny * 2 * kc
            out = dot(wx[p, jjs[0] * per_jj:(jjs[-1] + 1) * per_jj], jnp.concatenate(folded, axis=1), ((1,), (1,)))
            for u in range(GROUP):
                blocks = swap_rows(out[:, 2 * u * LANES:(2 * u + 1) * LANES],
                                   out[:, (2 * u + 1) * LANES:(2 * u + 2) * LANES])
                for jj in jjs:
                    for to in range(ny):
                        r = (jj - jjs[0]) * ny + to
                        at = (p * HALF_X_CHUNKS + jj) * crow + to * xrow + (group * GROUP + u) * 8
                        abuf[pl.ds(pl.multiple_of(at, 8), 8), :] = blocks[r % 2][r // 2]
            if p == 0 and jjs[0] == 0:
                for start, count in sends:
                    @pl.when(group == start + count - 1)
                    def _():
                        if start == 0:
                            pl.semaphore_wait(barrier, ny + nz - 2)
                        for o in x_offsets:
                            xf(0, o, start * GROUP * 8, count * GROUP * 8).start()
            return carry

        lax.fori_loop(first, stop, body, 0)

    def y_forward(j):
        own(abuf, bbuf, j, py, xrow)
        base = j * crow
        parts = []
        for c in range(2):
            parts.append(jnp.concatenate(
                [bbuf[pl.ds(base + 2 * i + c, n, stride=2 * kc), :] for i in range(2)], axis=1))
        for p in range(2):
            folded = jnp.concatenate([v[:half] - v[half:] if p else v[:half] + v[half:] for v in parts], axis=0)
            out = dot(wy[p], folded)
            for c in range(2):
                for to in range(nz):
                    for k in range(2):
                        at = base + to * yrow + (c * kc + k) * zl + p
                        abuf[pl.ds(at, zl // 2, stride=2), :] = out[
                            c * half + to * zl // 2:c * half + (to + 1) * zl // 2, k * LANES:(k + 1) * LANES]

    def z_solve(j):
        own(abuf, cbuf, j, pz, yrow)
        base, slot = j * crow, lax.rem(j, 2)
        p, jj = j // HALF_X_CHUNKS, lax.rem(j, HALF_X_CHUNKS)
        rows = kc * zl
        left = lax.broadcasted_iota(jnp.int32, (rows, LANES), 1) < zl
        swap = lambda v: pltpu.roll(v, zl, 1)
        lines = ([], [])
        for b in range(nz):
            at = base + b * yrow
            re = cbuf[pl.ds(pl.multiple_of(at, 8), rows), :]
            im = cbuf[pl.ds(pl.multiple_of(at + rows, 8), rows), :]
            lines[0].append(jnp.where(left, re, swap(im)))
            lines[1].append(jnp.where(left, swap(re), im))
        both = jnp.concatenate([jnp.concatenate(v, axis=1) for v in lines], axis=0)
        spec = dot(both, wz[...])
        gr = gbuf[slot, 0].reshape(rows, n)
        gi = gbuf[slot, 1].reshape(rows, n)
        scaled = []
        for f in range(nf):
            sr, si = spec[f * rows:(f + 1) * rows, :n], spec[f * rows:(f + 1) * rows, n:]
            hr, hi = sr * gr - si * gi, sr * gi + si * gr
            hat_re[f, pl.ds(kc * jj, kc), p] = hr.reshape(kc, zl, n)
            hat_im[f, pl.ds(kc * jj, kc), p] = hi.reshape(kc, zl, n)
            scaled.append(jnp.concatenate([hr, hi], axis=1))
        back = dot(jnp.concatenate(scaled, axis=0), wz[...], ((1,), (1,)))
        for b in range(nz):
            first, second = (back[f * rows:(f + 1) * rows, b * LANES:(b + 1) * LANES] for f in range(2))
            at = base + b * yrow
            cbuf[pl.ds(pl.multiple_of(at, 8), rows), :] = jnp.where(left, first, swap(second))
            cbuf[pl.ds(pl.multiple_of(at + rows, 8), rows), :] = jnp.where(left, swap(first), second)

    def y_inverse(j, i):
        base = j * crow
        halves = []
        for p in range(2):
            lines = jnp.concatenate(
                [dbuf[pl.ds(base + src * yrow + (c * kc + i) * zl + p, zl // 2, stride=2), :]
                 for c in range(2) for src in range(nz)], axis=0)
            halves.append(dot(wyi[p], lines))
        for s, out in enumerate((halves[0] + halves[1], halves[0] - halves[1])):
            for c in range(2):
                for to in range(ny // 2):
                    at = base + (s * (ny // 2) + to) * xrow + 2 * i * yl + c
                    bbuf[pl.ds(at, yl, stride=2), :] = out[c * half + to * yl:c * half + (to + 1) * yl]

    for c in range(2):
        rho_copy(c, 0).start()
    tables[0].start()
    for c in range(2):
        rho_copy(c, 1).start()
    for o in range(1, ny):
        pl.semaphore_signal(barrier, inc=1, device_id={"py": lax.rem(py + o, ny)}, device_id_type=MESH)
    for o in range(1, nz):
        pl.semaphore_signal(barrier, inc=1, device_id={"pz": lax.rem(pz + o, nz)}, device_id_type=MESH)
    tables[0].wait()
    x_forward(0, early, 0, groups)
    for c in range(2):
        g_copy(c, 0).start()
        g_copy(c, 1).start()
    for table in tables[1:]:
        table.start()
    x_prefetch(0)
    for jj in early[1:]:
        for o in x_offsets:
            xf(jj, o).start()
    for table in tables[1:]:
        table.wait()

    def step(t, carry):
        @pl.when(t < nj)
        def _():
            xf_wait(t)
            y_forward(t)
            for o in y_offsets:
                yf(t, o).start()

        @pl.when((t >= 1) & (t < nj + 1))
        def _():
            j = t - 1
            yf_wait(j)
            for c in range(2):
                g_copy(c, j).wait()
            z_solve(j)
            for i in range(kc):
                for o in y_offsets:
                    for c in range(2):
                        yi(j, o, (c * kc + i) * zl, zl, i).start()

            @pl.when(j + 2 < nj)
            def _():
                for c in range(2):
                    g_copy(c, j + 2).start()

        @pl.when(t >= 2)
        def _():
            j = t - 2
            own(cbuf, dbuf, j, pz, yrow)
            for i in range(kc):
                yi_wait(j, i)
                y_inverse(j, i)
                for o in x_offsets:
                    xi(j, o, 2 * i * yl, 2 * yl, jnp.where(j < cuts[1], 0, jnp.where(j < cuts[2], 1, 2))).start()
            own(bbuf, ebuf, j, py, xrow)

        def spare(p, jjs, begin):
            part = groups // 2

            def send(j, c):
                for o in x_offsets:
                    xf(j, o).start()
                return c

            @pl.when((t >= begin) & (t < begin + 2))
            def _():
                x_forward(p, jjs, (t - begin) * part, (t - begin + 1) * part)
                if p == 0:
                    x_prefetch(jnp.where(t == begin, part, 0))
                else:
                    @pl.when(t == begin)
                    def _():
                        x_prefetch(part)

            @pl.when(t == begin + 1)
            def _():
                base = p * HALF_X_CHUNKS
                lax.fori_loop(base + jjs[0], base + jjs[-1] + 1, send, 0)

        spare(0, late, 0)
        spare(1, odd, 2)

        @pl.when(t == nj - 4)
        def _():
            xi_wait(0)

        @pl.when((t >= nj - 4) & (t < nj))
        def _():
            def body(group, c):
                e = x_inverse(ebuf, wx, 0, odd, group, ny, crow, xrow)
                for c2 in range(2):
                    abuf[part_rows(0, group, c2, crow), :] = e[:, c2 * half:(c2 + 1) * half]
                return c

            first = (t - (nj - 4)) * piece
            lax.fori_loop(first, first + piece, body, 0)

        @pl.when(t == nj - 1)
        def _():
            xi_wait(1)
            lax.fori_loop(0, REFINE_EARLY, refine, 0)

        return carry

    def refine(group, carry):
        o = x_inverse(ebuf, wx, 1, range(SPLIT), group, ny, crow, xrow)
        for c in range(2):
            e, oc = abuf[part_rows(0, group, c, crow), :], o[:, c * half:(c + 1) * half]
            abuf[part_rows(0, group, c, crow), :] = e + oc
            abuf[part_rows(1, group, c, crow), :] = e - oc
        return carry

    lax.fori_loop(0, nj + 2, step, 0)
    lax.fori_loop(REFINE_EARLY, groups, refine, 0)
    xi_wait(2)


def part_rows(sign, group, c, crow):
    return pl.ds(pl.multiple_of((sign * HALF_X_CHUNKS + group) * crow + c * (crow // 2), 8), crow // 2)


def x_inverse(ebuf, wx, p, jjs, group, ny, crow, xrow):
    def tile(jj, src, i):
        at = (p * HALF_X_CHUNKS + jj) * crow + src * xrow + i * (xrow // 2) + group * 8
        return ebuf[pl.ds(pl.multiple_of(at, 8), 8), :]

    quads = [jnp.concatenate([tile(jj, src + k // 2, k % 2) for jj in jjs for src in range(0, ny, 2)], axis=0)
             for k in range(4)]
    a0, a2 = swap_rows(quads[0], quads[2])
    a1, a3 = swap_rows(quads[1], quads[3])
    lines = [v.reshape(-1, LANES) for v in (*swap_pairs(a0, a1), *swap_pairs(a2, a3))]
    per_jj = 4 * ny
    return dot(jnp.concatenate(lines, axis=1), wx[p, jjs[0] * per_jj:(jjs[-1] + 1) * per_jj], ((0,), (0,)))


def finish(ny, n, nf, ebuf, abuf, hat_re, hat_im, wx, phi_re, phi_im, out_re, out_im, stage, p_sem, h_sem):
    half = n // 2
    yl = n // ny
    nj = 2 * HALF_X_CHUNKS
    crow = ebuf.shape[0] // nj
    xrow = crow // ny
    zl = phi_re.shape[2]
    phi = (phi_re, phi_im)
    hats = [pltpu.make_async_copy(a, b, h_sem.at[c]) for c, (a, b) in enumerate(((hat_re, out_re), (hat_im, out_im)))]
    for h in hats:
        h.start()

    def phi_copy(c, group):
        slot = lax.rem(group, OUT_SLOTS)
        return pltpu.make_async_copy(stage.at[slot, c], phi[c].at[:, pl.ds(4 * group, 4)], p_sem.at[slot, c])

    def body(group, carry):
        @pl.when(group >= OUT_SLOTS)
        def _():
            for c in range(2):
                phi_copy(c, group - OUT_SLOTS).wait()

        slot = lax.rem(group, OUT_SLOTS)
        o = x_inverse(ebuf, wx, 1, range(SPLIT, HALF_X_CHUNKS), group, ny, crow, xrow)
        for c in range(2):
            low, high = (abuf[part_rows(sign, group, c, crow), :] for sign in range(2))
            oc = o[:, c * half:(c + 1) * half]
            out = jnp.concatenate([low + oc, high - oc], axis=1).reshape(4, nf, zl, n)
            stage[slot, c] = jnp.swapaxes(out, 0, 1)
        for c in range(2):
            phi_copy(c, group).start()
        return carry

    groups = yl // 4
    lax.fori_loop(0, groups, body, 0)
    for group in range(groups - OUT_SLOTS, groups):
        for c in range(2):
            phi_copy(c, group).wait()
    for h in hats:
        h.wait()


def solution(mesh):
    ny, nz = mesh.shape["py"], mesh.shape["pz"]

    def local_solve(rho_re, rho_im, g_re, g_im):
        nf, n, yl, zl = rho_re.shape
        kl, ml = g_re.shape[:2]
        kc = kl // HALF_X_CHUNKS // 2
        nj = 2 * HALF_X_CHUNKS
        rows = nj * ny * yl * 2 * kc
        tables = [jnp.asarray(w) for w in dft_tables(n, ny, nz)]
        space = jax.ShapeDtypeStruct((nf, yl, zl, n), jnp.float32)
        wave_shape = (nf, kl // 2, 2, ml, n)
        wave = jax.ShapeDtypeStruct(wave_shape, jnp.float32)
        dma = pltpu.SemaphoreType.DMA
        buf = pltpu.VMEM((rows, LANES), jnp.float32)
        vmem = pl.BlockSpec(memory_space=pltpu.VMEM)
        hbm = pl.BlockSpec(memory_space=pl.ANY)
        inner = pl.pallas_call(
            functools.partial(kernel, ny, nz, n, nf),
            out_shape=(pltpu.VMEM((rows, LANES), jnp.float32), pltpu.VMEM((rows, LANES), jnp.float32),
                       pltpu.VMEM(wave_shape, jnp.float32), pltpu.VMEM(wave_shape, jnp.float32)),
            in_specs=[hbm] * 8,
            out_specs=[vmem] * 4,
            scratch_shapes=[
                buf, buf, buf,
                pltpu.VMEM((SLOTS, 2, nf, 2 * GROUP, zl, n), jnp.float32),
                pltpu.VMEM((2, 2, kc, ml, n), jnp.float32),
                *[pltpu.VMEM(t.shape, jnp.float32) for t in tables],
                dma((nj,)), dma((nj,)), dma((DEPTH,)), dma((DEPTH,)),
                dma((DEPTH, kc)), dma((DEPTH, kc)), dma((3,)), dma((3,)),
                dma((len(tables),)), dma((SLOTS, 2)), dma((2, 2)),
            ],
            compiler_params=pltpu.CompilerParams(
                collective_id=0, has_side_effects=True, vmem_limit_bytes=INNER_VMEM),
            name="spectral",
        )(jnp.transpose(rho_re, (0, 2, 3, 1)), jnp.transpose(rho_im, (0, 2, 3, 1)),
          g_re.reshape(kl // 2, 2, ml, n), g_im.reshape(kl // 2, 2, ml, n), *tables)
        outs = pl.pallas_call(
            functools.partial(finish, ny, n, nf),
            out_shape=(space, space, wave, wave),
            in_specs=[vmem] * 5,
            out_specs=[hbm] * 4,
            scratch_shapes=[pltpu.VMEM((OUT_SLOTS, 2, nf, 4, zl, n), jnp.float32), dma((OUT_SLOTS, 2)), dma((2,))],
            compiler_params=pltpu.CompilerParams(vmem_limit_bytes=8 << 20),
            name="finish",
        )(*inner, tables[0])
        phi = [jnp.transpose(v, (0, 3, 1, 2)) for v in outs[:2]]
        return (*phi, *(v.reshape(nf, kl, ml, n) for v in outs[2:]))

    space_layout = P("dp", None, "py", "pz")
    wave_layout = P("dp", "py", "pz", None)
    green_layout = P("py", "pz", None)
    return jax.shard_map(local_solve, mesh=mesh,
                         in_specs=(space_layout, space_layout, green_layout, green_layout),
                         out_specs=(space_layout, space_layout, wave_layout, wave_layout),
                         check_vma=False)
```
